8 devices in a mesh: dp: 1 (over z), tp: 8 (over y, x, core).
Axes of the slice: x: 2, y: 2, z: 1, core: 2. Of those that a mesh axis runs over, the one named last changes fastest.
Arguments:
- y_one: float32 [16, 32, 3072], P('dp')
- y_two: float32 [16, 32, 3072], P('dp')
- dy_one: float32 [16, 32, 3072], P('dp')
- dy_two: float32 [16, 32, 3072], P('dp')
- seq_lens: int32 [16], P('dp')
- w_query: bfloat16 [3, 3072, 24, 128], P(None, None, 'tp')
- w_key: bfloat16 [3, 3072, 8, 128], P(None, None, 'tp')
- w_value: bfloat16 [3, 3072, 8, 128], P(None, None, 'tp')
- w_out: bfloat16 [3, 24, 128, 3072], P(None, 'tp')
- w_up: bfloat16 [3, 3072, 8192], P(None, None, 'tp')
- w_down: bfloat16 [3, 8192, 3072], P(None, 'tp')
Outputs:
- output 1: float32 [16, 32, 3072], P('dp')
- output 2: float32 [16, 32, 3072], P('dp')
- output 3: float32 [16, 32, 3072], P('dp')
- output 4: float32 [16, 32, 3072], P('dp')
- output 5: float32 [3, 3072, 24, 128], P('dp', None, 'tp')
- output 6: float32 [3, 3072, 8, 128], P('dp', None, 'tp')
- output 7: float32 [3, 3072, 8, 128], P('dp', None, 'tp')
- output 8: float32 [3, 24, 128, 3072], P('dp', 'tp')
- output 9: float32 [3, 3072, 8192], P('dp', None, 'tp')
- output 10: float32 [3, 8192, 3072], P('dp', 'tp')
All inputs are finite; a program needn't handle non-finite values.
Results may differ from the reference program's by a relative error of at most 0.02.
Values are sent between devices in bfloat16 or wider.
A program may use at most 1 GiB of HBM per device.

```python
import functools
import jax
import jax.numpy as jnp
from jax import lax

D = 3072
HEADS = 24
KV_HEADS = 8
HEAD = 128
FF = 8192
LAYERS = 3
SEQS = 2
SEQ = 32
TP = 8
KV_SLOTS = max(KV_HEADS, TP)
REPEAT = KV_SLOTS // KV_HEADS
GROUP = HEADS // KV_SLOTS
BATCH = SEQS * TP
TOKENS = BATCH * SEQ
EPS = 1e-5
SCORE_SCALE = HEAD ** -0.5
OUT_GAIN = 0.5 * (SEQ / 64) ** 0.25


def normal_weights(rng_key, arr_shape, scale_std):
    return (jax.random.normal(rng_key, arr_shape, jnp.float32) * scale_std).astype(jnp.bfloat16)


def draw_lengths(rng_key):
    len_key, top_key, low_key = jax.random.split(rng_key, 3)
    seq_lens = jax.random.randint(len_key, (BATCH,), SEQ // 4, SEQ + 1)
    top_idx = jax.random.randint(top_key, (), 0, BATCH)
    low_idx = (top_idx + jax.random.randint(low_key, (), 1, BATCH)) % BATCH
    positions = jnp.arange(BATCH)
    seq_lens = jnp.where(positions == top_idx, SEQ, seq_lens)
    seq_lens = jnp.where(positions == low_idx, SEQ // 4, seq_lens)
    return seq_lens.astype(jnp.int32)


def setup_inputs(seed: int = 0, part: int = 0) -> dict:
    weight_keys = jax.random.split(jax.random.key(seed), 6)
    part_keys = jax.random.split(jax.random.fold_in(jax.random.key(seed + 1), part), 5)
    act_shape = (BATCH, SEQ, D)
    key_heads = normal_weights(weight_keys[1], (LAYERS, D, KV_HEADS, HEAD), D ** -0.5)
    value_heads = normal_weights(weight_keys[2], (LAYERS, D, KV_HEADS, HEAD), D ** -0.5)
    return {
        'y_one': jax.random.normal(part_keys[0], act_shape, jnp.float32),
        'y_two': jax.random.normal(part_keys[1], act_shape, jnp.float32),
        'dy_one': jax.random.normal(part_keys[2], act_shape, jnp.float32),
        'dy_two': jax.random.normal(part_keys[3], act_shape, jnp.float32),
        'seq_lens': draw_lengths(part_keys[4]),
        'w_query': normal_weights(weight_keys[0], (LAYERS, D, HEADS, HEAD), 2.0 * D ** -0.5),
        'w_key': jnp.repeat(key_heads, REPEAT, axis=2),
        'w_value': jnp.repeat(value_heads, REPEAT, axis=2),
        'w_out': normal_weights(weight_keys[3], (LAYERS, HEADS, HEAD, D), OUT_GAIN * (HEADS * HEAD) ** -0.5),
        'w_up': normal_weights(weight_keys[4], (LAYERS, D, FF), D ** -0.5),
        'w_down': normal_weights(weight_keys[5], (LAYERS, FF, D), 0.6 * FF ** -0.5),
    }


def rms_norm(x_val):
    inv_rms = lax.rsqrt(jnp.mean(x_val * x_val, axis=-1, keepdims=True) + EPS)
    return x_val * inv_rms, inv_rms


def rms_back(normed, inv_rms, grad_norm):
    return inv_rms * (grad_norm - normed * jnp.mean(grad_norm * normed, axis=-1, keepdims=True))


def attend_seq(operands):
    q_seq, k_seq, v_seq, dout_seq, seq_len = operands
    q_grp = q_seq.reshape(SEQ, KV_SLOTS, GROUP, HEAD).astype(jnp.float32)
    k_full = k_seq.astype(jnp.float32)
    v_full = v_seq.astype(jnp.float32)
    dout_grp = dout_seq.reshape(SEQ, KV_SLOTS, GROUP, HEAD).astype(jnp.float32)
    row_pos = jnp.arange(SEQ)[:, None]
    col_pos = jnp.arange(SEQ)[None, :]
    visible = (col_pos <= row_pos) & (col_pos < seq_len)
    scores = jnp.einsum('igre,jge->grij', q_grp, k_full) * SCORE_SCALE
    scores = jnp.where(visible, scores, -1e30)
    attn_probs = jax.nn.softmax(scores, axis=-1)
    probs_b = attn_probs.astype(jnp.bfloat16).astype(jnp.float32)
    attn_out = jnp.einsum('grij,jge->igre', probs_b, v_full).astype(jnp.bfloat16)
    d_value = jnp.einsum('grij,igre->jge', probs_b, dout_grp).astype(jnp.bfloat16)
    d_probs = jnp.einsum('igre,jge->grij', dout_grp, v_full)
    d_scores = attn_probs * (d_probs - jnp.sum(d_probs * attn_probs, axis=-1, keepdims=True)) * SCORE_SCALE
    d_scores = d_scores.astype(jnp.bfloat16).astype(jnp.float32)
    d_query = jnp.einsum('grij,jge->igre', d_scores, k_full).astype(jnp.bfloat16)
    d_key = jnp.einsum('grij,igre->jge', d_scores, q_grp).astype(jnp.bfloat16)
    return attn_out.reshape(SEQ, HEADS, HEAD), d_query.reshape(SEQ, HEADS, HEAD), d_key, d_value


def layer_back(seq_lens, carry, layer_w):
    y_one, y_two, dy_one, dy_two = carry
    w_query, w_key, w_value, w_out, w_up, w_down = layer_w
    norm_g, inv_g = rms_norm(y_one.reshape(TOKENS, D))
    norm_g_b = norm_g.astype(jnp.bfloat16)
    pre_act = jnp.dot(norm_g_b, w_up, preferred_element_type=jnp.float32)
    act_val, gelu_back = jax.vjp(jax.nn.gelu, pre_act)
    act_b = act_val.astype(jnp.bfloat16)
    g_branch = jnp.dot(act_b, w_down, preferred_element_type=jnp.float32)
    x_two = y_two - g_branch.reshape(BATCH, SEQ, D)
    dy2_b = dy_two.reshape(TOKENS, D).astype(jnp.bfloat16)
    d_act = jnp.dot(dy2_b, w_down.T, preferred_element_type=jnp.float32)
    d_pre = gelu_back(d_act)[0].astype(jnp.bfloat16)
    dw_down = jnp.dot(act_b.T, dy2_b, preferred_element_type=jnp.float32)
    dw_up = jnp.dot(norm_g_b.T, d_pre, preferred_element_type=jnp.float32)
    grad_norm_g = jnp.dot(d_pre, w_up.T, preferred_element_type=jnp.float32)
    dy_one = dy_one + rms_back(norm_g, inv_g, grad_norm_g).reshape(BATCH, SEQ, D)

    norm_f, inv_f = rms_norm(x_two.reshape(TOKENS, D))
    norm_f_b = norm_f.astype(jnp.bfloat16)
    wq_flat = w_query.reshape(D, HEADS * HEAD)
    wk_flat = w_key.reshape(D, KV_SLOTS * HEAD)
    wv_flat = w_value.reshape(D, KV_SLOTS * HEAD)
    wo_flat = w_out.reshape(HEADS * HEAD, D)
    q_all = jnp.dot(norm_f_b, wq_flat, preferred_element_type=jnp.float32).astype(jnp.bfloat16).reshape(BATCH, SEQ, HEADS, HEAD)
    k_all = jnp.dot(norm_f_b, wk_flat, preferred_element_type=jnp.float32).astype(jnp.bfloat16).reshape(BATCH, SEQ, KV_SLOTS, HEAD)
    v_all = jnp.dot(norm_f_b, wv_flat, preferred_element_type=jnp.float32).astype(jnp.bfloat16).reshape(BATCH, SEQ, KV_SLOTS, HEAD)
    dy1_b = dy_one.reshape(TOKENS, D).astype(jnp.bfloat16)
    d_attn = jnp.dot(dy1_b, wo_flat.T, preferred_element_type=jnp.float32).astype(jnp.bfloat16).reshape(BATCH, SEQ, HEADS, HEAD)
    attn_out, d_query, d_key, d_value = lax.map(attend_seq, (q_all, k_all, v_all, d_attn, seq_lens))
    out_flat = attn_out.reshape(TOKENS, HEADS * HEAD)
    f_branch = jnp.dot(out_flat, wo_flat, preferred_element_type=jnp.float32)
    x_one = y_one - f_branch.reshape(BATCH, SEQ, D)
    dw_out = jnp.dot(out_flat.T, dy1_b, preferred_element_type=jnp.float32).reshape(HEADS, HEAD, D)
    dq_flat = d_query.reshape(TOKENS, HEADS * HEAD)
    dk_flat = d_key.reshape(TOKENS, KV_SLOTS * HEAD)
    dv_flat = d_value.reshape(TOKENS, KV_SLOTS * HEAD)
    dw_query = jnp.dot(norm_f_b.T, dq_flat, preferred_element_type=jnp.float32).reshape(D, HEADS, HEAD)
    dw_key = jnp.dot(norm_f_b.T, dk_flat, preferred_element_type=jnp.float32).reshape(D, KV_SLOTS, HEAD)
    dw_value = jnp.dot(norm_f_b.T, dv_flat, preferred_element_type=jnp.float32).reshape(D, KV_SLOTS, HEAD)
    grad_norm_f = (jnp.dot(dq_flat, wq_flat.T, preferred_element_type=jnp.float32)
                   + jnp.dot(dk_flat, wk_flat.T, preferred_element_type=jnp.float32)
                   + jnp.dot(dv_flat, wv_flat.T, preferred_element_type=jnp.float32))
    dx_two = dy_two + rms_back(norm_f, inv_f, grad_norm_f).reshape(BATCH, SEQ, D)
    return (x_one, x_two, dy_one, dx_two), (dw_query, dw_key, dw_value, dw_out, dw_up, dw_down)


def reference(y_one, y_two, dy_one, dy_two, seq_lens, w_query, w_key, w_value, w_out, w_up, w_down):
    end_state, layer_grads = lax.scan(functools.partial(layer_back, seq_lens), (y_one, y_two, dy_one, dy_two), (w_query, w_key, w_value, w_out, w_up, w_down), reverse=True)
    return (end_state[0], end_state[1], end_state[2], end_state[3], layer_grads[0], layer_grads[1], layer_grads[2], layer_grads[3], layer_grads[4], layer_grads[5])
```

```python
import functools

import jax
import jax.numpy as jnp
from jax import lax
from jax.experimental import pallas as pl
from jax.experimental.pallas import tpu as pltpu
from jax.sharding import PartitionSpec as P

F32 = jnp.float32
BF16 = jnp.bfloat16
EPS = 1e-5
MASK_VALUE = -1e30
MESH = pl.DeviceIdType.MESH
TILE = 128
N_TILES = 4
GELU_C = 0.7978845608028654
GELU_A = 0.044715
OWNER = (0, 4, 2, 6, 1, 3, 5, 7)
ORDER = (('e', 3), ('g', 4), ('C', 0), ('f', 3), ('b', 0), ('c', 1), ('d', 2))


def dot_nn(lhs, rhs):
    return lax.dot_general(lhs, rhs, (((1,), (0,)), ((), ())), preferred_element_type=F32)


def dot_nt(lhs, rhs):
    return lax.dot_general(lhs, rhs, (((1,), (1,)), ((), ())), preferred_element_type=F32)


def dot_tn(lhs, rhs):
    return lax.dot_general(lhs, rhs, (((0,), (0,)), ((), ())), preferred_element_type=F32)


def inv_rms_of(x_val):
    return lax.rsqrt(jnp.mean(x_val * x_val, axis=-1, keepdims=True) + EPS)


def stack_kernel(n_layers, width, ff, qw, kw,
                 ne0, mask, y_one, y_two, dy_one, dy_two, w_qkv, w_out, w_up, w_down,
                 o_state, o_ng, o_eg, o_h, o_u, o_nf, o_ef, o_a, o_dq, o_dk, o_dv,
                 ne, part, rec_d, rec_one, rec_two, x_st, d_st, wu, wd, wqkv, wo, h_buf, u_buf,
                 a_buf, dqkv_buf, q_buf, send_sem, recv_sem, w_sem, in_sem, out_sem):
    n_steps = 2 * n_layers * N_TILES
    me = lax.axis_index('tp')
    core = me % 2
    x_pos = (me // 2) % 2
    y_pos = me // 4
    mate = me + 1 - 2 * core
    x_peer = me + 2 - 4 * x_pos
    y_peer = me + 4 - 8 * y_pos
    peer_one = x_peer * (1 - core) + y_peer * core
    peer_two = y_peer * (1 - core) + x_peer * core
    bit_one = x_pos * (1 - core) + y_pos * core
    bit_two = y_pos * (1 - core) + x_pos * core
    half = pl.multiple_of(core * 64, 64)
    half_other = pl.multiple_of(64 - core * 64, 64)
    quarter = pl.multiple_of(half + bit_one * 32, 32)
    quarter_other = pl.multiple_of(half + 32 - bit_one * 32, 32)
    own = pl.multiple_of(quarter + bit_two * 16, 16)
    own_other = pl.multiple_of(quarter + 16 - bit_two * 16, 16)

    def mlp_loads(layer):
        return (pltpu.make_async_copy(w_up.at[layer], wu, w_sem.at[0]),
                pltpu.make_async_copy(w_down.at[layer], wd, w_sem.at[1]))

    def attn_loads(layer):
        return (pltpu.make_async_copy(w_qkv.at[layer], wqkv, w_sem.at[2]),
                pltpu.make_async_copy(w_out.at[layer], wo, w_sem.at[3]))

    in_copies = [pltpu.make_async_copy(ne0, ne, in_sem.at[0])]
    for pos, (src, dst) in enumerate(((y_one, x_st.at[0]), (y_two, x_st.at[1]),
                                      (dy_one, d_st.at[0]), (dy_two, d_st.at[1]))):
        for tile in range(N_TILES):
            in_copies.append(pltpu.make_async_copy(
                src.at[pl.ds(tile * TILE + own, 16), :], dst.at[tile], in_sem.at[1 + pos * N_TILES + tile]))
    for copy in mlp_loads(n_layers - 1):
        copy.start()
    for copy in in_copies:
        copy.start()
    for copy in attn_loads(n_layers - 1):
        copy.start()

    barrier = pltpu.get_barrier_semaphore()
    for peer in (mate, x_peer, y_peer):
        pl.semaphore_signal(barrier, inc=1, device_id={'tp': peer}, device_id_type=MESH)
    pl.semaphore_wait(barrier, 3)
    for copy in in_copies:
        copy.wait()

    def remote(stage, tile):
        src, dst, peer = {
            0: lambda: (part.at[tile, :, pl.ds(half_other, 64), :], rec_d.at[tile], mate),
            1: lambda: (part.at[tile, :, pl.ds(quarter_other, 32), :], rec_one.at[tile], peer_one),
            2: lambda: (part.at[tile, :, pl.ds(own_other, 16), :], rec_two.at[tile], peer_two),
            3: lambda: (ne.at[tile, :, pl.ds(own, 16), :], ne.at[tile, :, pl.ds(own, 16), :], peer_two),
            4: lambda: (ne.at[tile, :, pl.ds(quarter, 32), :], ne.at[tile, :, pl.ds(quarter, 32), :], peer_one),
            5: lambda: (ne.at[tile, :, pl.ds(half, 64), :], ne.at[tile, :, pl.ds(half, 64), :], mate),
        }[stage]()
        return pltpu.make_async_remote_copy(
            src_ref=src, dst_ref=dst, send_sem=send_sem.at[tile, stage], recv_sem=recv_sem.at[tile, stage],
            device_id={'tp': peer}, device_id_type=MESH)

    def mlp_tile(layer, tile):
        rows = pl.ds(tile * TILE, TILE)
        saves = [pltpu.make_async_copy(ne.at[tile, 0], o_ng.at[layer, rows, :], out_sem.at[0]),
                 pltpu.make_async_copy(ne.at[tile, 1], o_eg.at[layer, rows, :], out_sem.at[1])]
        for copy in saves:
            copy.start()

        @pl.when(tile == 0)
        def _():
            for copy in mlp_loads(layer):
                copy.wait()

        @pl.loop(0, ff // 256)
        def _(pos):
            cols = pl.ds(pl.multiple_of(pos * 256, 256), 256)
            pre = dot_nn(ne[tile, 0], wu[:, cols])
            d_act = dot_nt(ne[tile, 1], wd[cols, :])
            tanh_val = jnp.tanh(GELU_C * (pre + GELU_A * (pre * pre * pre)))
            h_buf[:, cols] = (0.5 * pre * (1.0 + tanh_val)).astype(BF16)
            slope = 0.5 * (1.0 + tanh_val) + (0.5 * GELU_C) * pre * (1.0 - tanh_val * tanh_val) * (1.0 + (3.0 * GELU_A) * (pre * pre))
            u_buf[:, cols] = (slope * d_act).astype(BF16)

        more = [pltpu.make_async_copy(h_buf, o_h.at[layer, rows, :], out_sem.at[2]),
                pltpu.make_async_copy(u_buf, o_u.at[layer, rows, :], out_sem.at[3])]
        for copy in more:
            copy.start()

        @pl.loop(0, width // 512)
        def _(pos):
            cols = pl.ds(pl.multiple_of(pos * 512, 512), 512)
            part[tile, 0, :, cols] = dot_nn(h_buf[...], wd[:, cols])
            part[tile, 1, :, cols] = dot_nt(u_buf[...], wu[cols, :])

        for copy in saves + more:
            copy.wait()

        @pl.when((tile == N_TILES - 1) & (layer > 0))
        def _():
            for copy in mlp_loads(layer - 1):
                copy.start()

    def attn_tile(layer, tile):
        rows = pl.ds(tile * TILE, TILE)
        saves = [pltpu.make_async_copy(ne.at[tile, 0], o_nf.at[layer, rows, :], out_sem.at[0]),
                 pltpu.make_async_copy(ne.at[tile, 1], o_ef.at[layer, rows, :], out_sem.at[1])]
        for copy in saves:
            copy.start()

        @pl.when(tile == 0)
        def _():
            for copy in attn_loads(layer):
                copy.wait()

        n_val = ne[tile, 0]
        q_buf[:, :qw] = dot_nn(n_val, wqkv[:, :qw]).astype(BF16)
        q_buf[:, qw:] = dot_nn(n_val, wqkv[:, qw:]).astype(BF16)
        key = q_buf[:, qw:qw + kw]
        value = q_buf[:, qw + kw:]
        d_attn_all = dot_nt(ne[tile, 1], wo[...]).astype(BF16)
        visible = mask[tile] > 0.5
        scale = kw ** -0.5
        d_key = jnp.zeros((TILE, kw), F32)
        d_value = jnp.zeros((TILE, kw), F32)
        for head in range(qw // kw):
            cols = slice(head * kw, (head + 1) * kw)
            query = q_buf[:, cols]
            d_attn = d_attn_all[:, cols]
            scores = jnp.where(visible, dot_nt(query, key) * scale, MASK_VALUE)
            weights = jnp.exp(scores - jnp.max(scores, axis=-1, keepdims=True))
            probs = weights / jnp.sum(weights, axis=-1, keepdims=True)
            probs_b = probs.astype(BF16)
            a_buf[:, cols] = dot_nn(probs_b, value).astype(BF16)
            d_value += dot_tn(probs_b, d_attn)
            d_probs = dot_nt(d_attn, value)
            d_scores = (probs * (d_probs - jnp.sum(d_probs * probs, axis=-1, keepdims=True)) * scale).astype(BF16)
            dqkv_buf[:, cols] = dot_nn(d_scores, key).astype(BF16)
            d_key += dot_tn(d_scores, query)
        dqkv_buf[:, qw:qw + kw] = d_key.astype(BF16)
        dqkv_buf[:, qw + kw:] = d_value.astype(BF16)

        more = [pltpu.make_async_copy(a_buf, o_a.at[layer, rows, :], out_sem.at[2]),
                pltpu.make_async_copy(dqkv_buf.at[:, :qw], o_dq.at[layer, rows, :], out_sem.at[3]),
                pltpu.make_async_copy(dqkv_buf.at[:, qw:qw + kw], o_dk.at[layer, rows, :], out_sem.at[4]),
                pltpu.make_async_copy(dqkv_buf.at[:, qw + kw:], o_dv.at[layer, rows, :], out_sem.at[5])]
        for copy in more:
            copy.start()

        @pl.loop(0, width // 512)
        def _(pos):
            cols = pl.ds(pl.multiple_of(pos * 512, 512), 512)
            part[tile, 0, :, cols] = dot_nn(a_buf[...], wo[:, cols])
            part[tile, 1, :, cols] = dot_nt(dqkv_buf[...], wqkv[cols, :])

        for copy in saves + more:
            copy.wait()

        @pl.when((tile == N_TILES - 1) & (layer > 0))
        def _():
            for copy in attn_loads(layer - 1):
                copy.start()

    def add_rows(tile, base, n_rows, received):
        for unit in range(2):
            @pl.loop(0, n_rows // 8)
            def _(pos):
                row = pl.multiple_of(pos * 8, 8)
                dst = pl.ds(pl.multiple_of(base + row, 8), 8)
                part[tile, unit, dst, :] += received[tile, unit, pl.ds(row, 8), :]

    def finish_rows(branch, tile):
        rows = pl.ds(own, 16)
        other = 1 - branch
        x_new = x_st[other, tile] - (part[tile, 0, rows, :] + rec_two[tile, 0])
        x_st[other, tile] = x_new
        ne[tile, 0, rows, :] = (x_new * inv_rms_of(x_new)).astype(BF16)
        grad = part[tile, 1, rows, :] + rec_two[tile, 1]
        x_val = x_st[branch, tile]
        inv = inv_rms_of(x_val)
        normed = x_val * inv
        d_new = d_st[branch, tile] + inv * (grad - normed * jnp.mean(grad * normed, axis=-1, keepdims=True))
        d_st[branch, tile] = d_new
        ne[tile, 1, rows, :] = d_new.astype(BF16)

    def run_stage(stage, idx):
        tile = idx % N_TILES
        turn = idx // N_TILES
        branch = turn % 2
        layer = n_layers - 1 - turn // 2
        travels = idx < n_steps - N_TILES
        if stage == 'C':
            @pl.when(branch == 0)
            def _():
                mlp_tile(layer, tile)

            @pl.when(branch == 1)
            def _():
                attn_tile(layer, tile)
            remote(0, tile).start()
        elif stage == 'b':
            remote(0, tile).wait()
            add_rows(tile, half, 64, rec_d)
            remote(1, tile).start()
        elif stage == 'c':
            remote(1, tile).wait()
            add_rows(tile, quarter, 32, rec_one)
            remote(2, tile).start()
        elif stage == 'd':
            remote(2, tile).wait()
            finish_rows(branch, tile)

            @pl.when(travels)
            def _():
                remote(3, tile).start()
        elif stage == 'e':
            @pl.when(travels)
            def _():
                remote(3, tile).wait()
                remote(4, tile).start()
        elif stage == 'f':
            @pl.when(travels)
            def _():
                remote(4, tile).wait()
                remote(5, tile).start()
        else:
            @pl.when(travels)
            def _():
                remote(5, tile).wait()

    max_lag = max(lag for _, lag in ORDER)

    @pl.loop(0, n_steps + max_lag)
    def _(step):
        for stage, lag in ORDER:
            @pl.when((step >= lag) & (step < n_steps + lag))
            def _():
                run_stage(stage, step - lag)

    finals = []
    for pos, src in enumerate((x_st.at[0], x_st.at[1], d_st.at[0], d_st.at[1])):
        finals.append(pltpu.make_async_copy(src, o_state.at[pos], out_sem.at[pos]))
    for copy in finals:
        copy.start()
    for copy in finals:
        copy.wait()


def run_stack(ne0, mask, y_one, y_two, dy_one, dy_two, w_qkv, w_out, w_up, w_down):
    n_layers, width, ff = w_up.shape
    qw = w_out.shape[1]
    kw = (w_qkv.shape[2] - qw) // 2
    tokens = y_one.shape[0]
    any_spec = pl.BlockSpec(memory_space=pl.ANY)
    out = lambda *shape: jax.ShapeDtypeStruct((n_layers, tokens) + shape, BF16)
    return pl.pallas_call(
        functools.partial(stack_kernel, n_layers, width, ff, qw, kw),
        out_shape=(jax.ShapeDtypeStruct((4, N_TILES, 16, width), F32),
                   out(width), out(width), out(ff), out(ff), out(width), out(width),
                   out(qw), out(qw), out(kw), out(kw)),
        in_specs=[any_spec, pl.BlockSpec(memory_space=pltpu.VMEM)] + [any_spec] * 8,
        out_specs=(any_spec,) * 11,
        scratch_shapes=[
            pltpu.VMEM((N_TILES, 2, TILE, width), BF16),
            pltpu.VMEM((N_TILES, 2, TILE, width), F32),
            pltpu.VMEM((N_TILES, 2, 64, width), F32),
            pltpu.VMEM((N_TILES, 2, 32, width), F32),
            pltpu.VMEM((N_TILES, 2, 16, width), F32),
            pltpu.VMEM((2, N_TILES, 16, width), F32),
            pltpu.VMEM((2, N_TILES, 16, width), F32),
            pltpu.VMEM((width, ff), BF16),
            pltpu.VMEM((ff, width), BF16),
            pltpu.VMEM((width, qw + 2 * kw), BF16),
            pltpu.VMEM((qw, width), BF16),
            pltpu.VMEM((TILE, ff), BF16),
            pltpu.VMEM((TILE, ff), BF16),
            pltpu.VMEM((TILE, qw), BF16),
            pltpu.VMEM((TILE, qw + 2 * kw), BF16),
            pltpu.VMEM((TILE, qw + 2 * kw), BF16),
            pltpu.SemaphoreType.DMA((N_TILES, 6)),
            pltpu.SemaphoreType.DMA((N_TILES, 6)),
            pltpu.SemaphoreType.DMA((4,)),
            pltpu.SemaphoreType.DMA((1 + 4 * N_TILES,)),
            pltpu.SemaphoreType.DMA((6,)),
        ],
        compiler_params=pltpu.CompilerParams(
            collective_id=0, has_side_effects=True, vmem_limit_bytes=67043328),
        name='stack',
    )(ne0, mask, y_one, y_two, dy_one, dy_two, w_qkv, w_out, w_up, w_down)


def tile_mask(seq_lens, seq_len):
    n_seq = TILE // seq_len
    row = lax.broadcasted_iota(jnp.int32, (N_TILES, TILE, TILE), 1)
    col = lax.broadcasted_iota(jnp.int32, (N_TILES, TILE, TILE), 2)
    lens = jnp.repeat(seq_lens.reshape(N_TILES, 1, n_seq), seq_len, axis=2)
    seen = (row // seq_len == col // seq_len) & (col <= row) & (col % seq_len < lens)
    return seen.astype(F32)


def solution(mesh):
    act_spec = P('dp', None, None)
    w_specs = (P(None, None, 'tp', None), P(None, None, 'tp', None), P(None, None, 'tp', None),
               P(None, 'tp', None, None), P(None, None, 'tp'), P(None, 'tp', None))
    g_specs = (P('dp', None, 'tp', None), P('dp', None, 'tp', None), P('dp', None, 'tp', None),
               P('dp', 'tp', None, None), P('dp', None, 'tp'), P('dp', 'tp', None))

    def local_fn(y_one, y_two, dy_one, dy_two, seq_lens, w_query, w_key, w_value, w_out, w_up, w_down):
        n_batch, seq_len, width = y_one.shape
        tokens = n_batch * seq_len
        n_layers, _, n_heads, head_dim = w_query.shape
        slots = w_key.shape[2]
        flat = lambda val: val.reshape(tokens, width)
        norm = (y_one * lax.rsqrt(jnp.mean(y_one * y_one, axis=-1, keepdims=True) + EPS)).astype(BF16)
        tiled = lambda val: val.astype(BF16).reshape(N_TILES, 1, TILE, width)
        ne0 = jnp.concatenate([tiled(norm), tiled(dy_two)], axis=1)
        w_qkv = jnp.concatenate([w_val.reshape(n_layers, width, -1) for w_val in (w_query, w_key, w_value)], axis=2)
        state, n_g, e_g, h_all, u_all, n_f, e_f, a_all, dq, dk, dv = run_stack(
            ne0, tile_mask(seq_lens, seq_len), flat(y_one), flat(y_two), flat(dy_one), flat(dy_two),
            w_qkv, w_out.reshape(n_layers, n_heads * head_dim, width), w_up, w_down)

        def whole(val):
            blocks = lax.all_gather(val, 'tp', axis=0)
            return jnp.stack([blocks[owner] for owner in OWNER], axis=1).reshape(n_batch, seq_len, width)

        finals = tuple(whole(state[pos]) for pos in range(4))
        heads = lambda val, count: val.reshape(n_layers, tokens, count, head_dim)
        dot = functools.partial(jnp.einsum, preferred_element_type=F32)
        dw_query = dot('ltd,lthe->ldhe', n_f, heads(dq, n_heads))
        dw_key = dot('ltd,lthe->ldhe', n_f, heads(dk, slots))
        dw_value = dot('ltd,lthe->ldhe', n_f, heads(dv, slots))
        dw_out = dot('lthe,ltd->lhed', heads(a_all, n_heads), e_f)
        dw_up = dot('ltd,ltf->ldf', n_g, u_all)
        dw_down = dot('ltf,ltd->lfd', h_all, e_g)
        return finals + (dw_query, dw_key, dw_value, dw_out, dw_up, dw_down)

    return jax.shard_map(local_fn, mesh=mesh,
                         in_specs=(act_spec,) * 4 + (P('dp'),) + w_specs,
                         out_specs=(act_spec,) * 4 + g_specs,
                         check_vma=False)
```

```python
import functools

import jax
import jax.numpy as jnp
from jax import lax
from jax.experimental import pallas as pl
from jax.experimental.pallas import tpu as pltpu
from jax.sharding import PartitionSpec as P

F32 = jnp.float32
BF16 = jnp.bfloat16
EPS = 1e-5
MASK_VALUE = -1e30
MESH = pl.DeviceIdType.MESH
TILE = 128
N_TILES = 4
GELU_C = 0.7978845608028654
GELU_A = 0.044715
ORDER = (('g', 4), ('C', 0), ('e', 3), ('c', 1), ('b', 0), ('f', 3), ('d', 2))


def dot_nn(lhs, rhs):
    return lax.dot_general(lhs, rhs, (((1,), (0,)), ((), ())), preferred_element_type=F32)


def dot_nt(lhs, rhs):
    return lax.dot_general(lhs, rhs, (((1,), (1,)), ((), ())), preferred_element_type=F32)


def dot_tn(lhs, rhs):
    return lax.dot_general(lhs, rhs, (((0,), (0,)), ((), ())), preferred_element_type=F32)


def inv_rms_of(x_val):
    return lax.rsqrt(jnp.mean(x_val * x_val, axis=-1, keepdims=True) + EPS)


def stack_kernel(n_layers, width, ff, qw, kw,
                 mask, y_one, y_two, dy_one, dy_two, w_query, w_key, w_value, w_out, w_up, w_down,
                 o_x1, o_dx2, o_x2, o_dy1, o_ng, o_eg, o_h, o_u, o_nf, o_ef, o_a, o_dq, o_dk, o_dv,
                 ne_bf, part, rec_d, rec_one, rec_two, x_st, d_st, wu, wd, wqkv, wo, h_buf, u_buf,
                 a_buf, dqkv_buf, q_buf, send_sem, recv_sem, w_sem, in_sem, act_sem, out_sem, free_sem):
    n_steps = 2 * n_layers * N_TILES
    me = lax.axis_index('tp')
    core = me % 2
    x_pos = (me // 2) % 2
    y_pos = me // 4
    mate = me + 1 - 2 * core
    x_peer = me + 2 - 4 * x_pos
    y_peer = me + 4 - 8 * y_pos
    peer_one = x_peer * (1 - core) + y_peer * core
    peer_two = y_peer * (1 - core) + x_peer * core
    bit_one = x_pos * (1 - core) + y_pos * core
    bit_two = y_pos * (1 - core) + x_pos * core
    half = pl.multiple_of(core * 64, 64)
    half_other = pl.multiple_of(64 - core * 64, 64)
    quarter = pl.multiple_of(half + bit_one * 32, 32)
    quarter_other = pl.multiple_of(half + 32 - bit_one * 32, 32)
    own = pl.multiple_of(quarter + bit_two * 16, 16)
    own_other = pl.multiple_of(quarter + 16 - bit_two * 16, 16)

    def mlp_loads(layer):
        return (pltpu.make_async_copy(w_up.at[layer], wu, w_sem.at[0]),
                pltpu.make_async_copy(w_down.at[layer], wd, w_sem.at[1]))

    def attn_loads(layer):
        heads = [w_query.at[layer, head] for head in range(qw // kw)]
        heads += [w_key.at[layer, 0], w_value.at[layer, 0]]
        copies = [pltpu.make_async_copy(src, wqkv.at[:, pl.ds(pos * kw, kw)], w_sem.at[3 + pos])
                  for pos, src in enumerate(heads)]
        return copies + [pltpu.make_async_copy(w_out.at[layer], wo, w_sem.at[2])]

    def act_loads(tile):
        rows = pl.ds(tile * TILE, TILE)
        return (pltpu.make_async_copy(y_one.at[rows, :], part.at[tile, 0], act_sem.at[tile, 0]),
                pltpu.make_async_copy(dy_two.at[rows, :], part.at[tile, 1], act_sem.at[tile, 1]))

    def own_loads(tile):
        pairs = ((y_one, x_st.at[0]), (y_two, x_st.at[1]), (dy_one, d_st.at[0]), (dy_two, d_st.at[1]))
        return [pltpu.make_async_copy(src.at[pl.ds(tile * TILE + own, 16), :], dst.at[tile], in_sem.at[pos, tile])
                for pos, (src, dst) in enumerate(pairs)]

    for copy in act_loads(0):
        copy.start()
    for copy in mlp_loads(n_layers - 1):
        copy.start()
    for tile in range(1, N_TILES):
        for copy in act_loads(tile):
            copy.start()
    for tile in range(N_TILES):
        for copy in own_loads(tile):
            copy.start()
    for copy in attn_loads(n_layers - 1):
        copy.start()

    barrier = pltpu.get_barrier_semaphore()
    for peer in (mate, x_peer, y_peer):
        pl.semaphore_signal(barrier, inc=1, device_id={'tp': peer}, device_id_type=MESH)
    pl.semaphore_wait(barrier, 3)

    def remote(stage, tile, wide=False):
        ne = part if wide else ne_bf
        src, dst, peer = {
            0: lambda: (part.at[tile, :, pl.ds(half_other, 64), :], rec_d.at[tile], mate),
            1: lambda: (part.at[tile, :, pl.ds(quarter_other, 32), :], rec_one.at[tile], peer_one),
            2: lambda: (part.at[tile, :, pl.ds(own_other, 16), :], rec_two.at[tile], peer_two),
            3: lambda: (ne.at[tile, :, pl.ds(own, 16), :], ne.at[tile, :, pl.ds(own, 16), :], peer_two),
            4: lambda: (ne.at[tile, :, pl.ds(quarter, 32), :], ne.at[tile, :, pl.ds(quarter, 32), :], peer_one),
            5: lambda: (ne.at[tile, :, pl.ds(half, 64), :], ne.at[tile, :, pl.ds(half, 64), :], mate),
        }[stage]()
        return pltpu.make_async_remote_copy(
            src_ref=src, dst_ref=dst, send_sem=send_sem.at[tile, stage], recv_sem=recv_sem.at[tile, stage],
            device_id={'tp': peer}, device_id_type=MESH)

    ne = ne_bf

    def convert(tile):
        @pl.loop(0, TILE // 16)
        def _(pos):
            rows = pl.ds(pl.multiple_of(pos * 16, 16), 16)
            x_val = part[tile, 0, rows, :]
            ne[tile, 0, rows, :] = (x_val * inv_rms_of(x_val)).astype(BF16)
            ne[tile, 1, rows, :] = part[tile, 1, rows, :].astype(BF16)

    def mlp_tile(layer, tile):
        @pl.when(layer == n_layers - 1)
        def _():
            for copy in act_loads(tile):
                copy.wait()
            convert(tile)


        rows = pl.ds(tile * TILE, TILE)
        saves = [pltpu.make_async_copy(ne.at[tile, 0], o_ng.at[layer, rows, :], out_sem.at[0]),
                 pltpu.make_async_copy(ne.at[tile, 1], o_eg.at[layer, rows, :], out_sem.at[1])]
        for copy in saves:
            copy.start()

        @pl.when(tile == 0)
        def _():
            for copy in mlp_loads(layer):
                copy.wait()

        @pl.loop(0, ff // 256)
        def _(pos):
            cols = pl.ds(pl.multiple_of(pos * 256, 256), 256)
            pre = dot_nn(ne[tile, 0], wu[:, cols])
            d_act = dot_nt(ne[tile, 1], wd[cols, :])
            tanh_val = jnp.tanh(GELU_C * (pre + GELU_A * (pre * pre * pre)))
            h_buf[:, cols] = (0.5 * pre * (1.0 + tanh_val)).astype(BF16)
            slope = 0.5 * (1.0 + tanh_val) + (0.5 * GELU_C) * pre * (1.0 - tanh_val * tanh_val) * (1.0 + (3.0 * GELU_A) * (pre * pre))
            u_buf[:, cols] = (slope * d_act).astype(BF16)

        more = [pltpu.make_async_copy(h_buf, o_h.at[layer, rows, :], out_sem.at[2]),
                pltpu.make_async_copy(u_buf, o_u.at[layer, rows, :], out_sem.at[3])]
        for copy in more:
            copy.start()

        @pl.loop(0, width // 512)
        def _(pos):
            cols = pl.ds(pl.multiple_of(pos * 512, 512), 512)
            part[tile, 0, :, cols] = dot_nn(h_buf[...], wd[:, cols])
            part[tile, 1, :, cols] = dot_nt(u_buf[...], wu[cols, :])

        for copy in saves + more:
            copy.wait()

        @pl.when((tile == N_TILES - 1) & (layer > 0))
        def _():
            for copy in mlp_loads(layer - 1):
                copy.start()

    def attn_tile(layer, tile):
        rows = pl.ds(tile * TILE, TILE)
        wide_saves = [pltpu.make_async_copy(part.at[tile, 0], o_x2.at[rows, :], out_sem.at[6]),
                      pltpu.make_async_copy(part.at[tile, 1], o_dy1.at[rows, :], out_sem.at[7])]

        @pl.when(layer == 0)
        def _():
            for copy in wide_saves:
                copy.start()
            convert(tile)

        saves = [pltpu.make_async_copy(ne.at[tile, 0], o_nf.at[layer, rows, :], out_sem.at[0]),
                 pltpu.make_async_copy(ne.at[tile, 1], o_ef.at[layer, rows, :], out_sem.at[1])]
        for copy in saves:
            copy.start()

        @pl.when(tile == 0)
        def _():
            for copy in attn_loads(layer):
                copy.wait()

        n_val = ne[tile, 0]
        q_buf[:, :qw] = dot_nn(n_val, wqkv[:, :qw]).astype(BF16)
        q_buf[:, qw:] = dot_nn(n_val, wqkv[:, qw:]).astype(BF16)
        key = q_buf[:, qw:qw + kw]
        value = q_buf[:, qw + kw:]
        d_attn_all = dot_nt(ne[tile, 1], wo[...]).astype(BF16)
        visible = mask[tile] > 0.5
        scale = kw ** -0.5
        d_key = jnp.zeros((TILE, kw), F32)
        d_value = jnp.zeros((TILE, kw), F32)
        for head in range(qw // kw):
            cols = slice(head * kw, (head + 1) * kw)
            query = q_buf[:, cols]
            d_attn = d_attn_all[:, cols]
            scores = jnp.where(visible, dot_nt(query, key) * scale, MASK_VALUE)
            weights = jnp.exp(scores - jnp.max(scores, axis=-1, keepdims=True))
            probs = weights / jnp.sum(weights, axis=-1, keepdims=True)
            probs_b = probs.astype(BF16)
            a_buf[:, cols] = dot_nn(probs_b, value).astype(BF16)
            d_value += dot_tn(probs_b, d_attn)
            d_probs = dot_nt(d_attn, value)
            d_scores = (probs * (d_probs - jnp.sum(d_probs * probs, axis=-1, keepdims=True)) * scale).astype(BF16)
            dqkv_buf[:, cols] = dot_nn(d_scores, key).astype(BF16)
            d_key += dot_tn(d_scores, query)
        dqkv_buf[:, qw:qw + kw] = d_key.astype(BF16)
        dqkv_buf[:, qw + kw:] = d_value.astype(BF16)

        more = [pltpu.make_async_copy(a_buf, o_a.at[layer, rows, :], out_sem.at[2]),
                pltpu.make_async_copy(dqkv_buf.at[:, :qw], o_dq.at[layer, rows, :], out_sem.at[3]),
                pltpu.make_async_copy(dqkv_buf.at[:, qw:qw + kw], o_dk.at[layer, rows, :], out_sem.at[4]),
                pltpu.make_async_copy(dqkv_buf.at[:, qw + kw:], o_dv.at[layer, rows, :], out_sem.at[5])]
        for copy in more:
            copy.start()

        @pl.when(layer == 0)
        def _():
            for copy in wide_saves:
                copy.wait()

        @pl.loop(0, width // 512)
        def _(pos):
            cols = pl.ds(pl.multiple_of(pos * 512, 512), 512)
            part[tile, 0, :, cols] = dot_nn(a_buf[...], wo[:, cols])
            part[tile, 1, :, cols] = dot_nt(dqkv_buf[...], wqkv[cols, :])

        for copy in saves + more:
            copy.wait()

        @pl.when((tile == N_TILES - 1) & (layer > 0))
        def _():
            for copy in attn_loads(layer - 1):
                copy.start()

    def add_rows(tile, base, n_rows, received):
        for unit in range(2):
            @pl.loop(0, n_rows // 8)
            def _(pos):
                row = pl.multiple_of(pos * 8, 8)
                dst = pl.ds(pl.multiple_of(base + row, 8), 8)
                part[tile, unit, dst, :] += received[tile, unit, pl.ds(row, 8), :]

    def finish_rows(branch, tile, wide):
        rows = pl.ds(own, 16)
        other = 1 - branch
        x_new = x_st[other, tile] - (part[tile, 0, rows, :] + rec_two[tile, 0])
        x_st[other, tile] = x_new
        grad = part[tile, 1, rows, :] + rec_two[tile, 1]
        x_val = x_st[branch, tile]
        inv = inv_rms_of(x_val)
        normed = x_val * inv
        d_new = d_st[branch, tile] + inv * (grad - normed * jnp.mean(grad * normed, axis=-1, keepdims=True))
        d_st[branch, tile] = d_new

        @pl.when(wide)
        def _():
            part[tile, 0, rows, :] = x_new
            part[tile, 1, rows, :] = d_new

        @pl.when(jnp.logical_not(wide))
        def _():
            ne[tile, 0, rows, :] = (x_new * inv_rms_of(x_new)).astype(BF16)
            ne[tile, 1, rows, :] = d_new.astype(BF16)

    def run_stage(stage, idx):
        tile = idx % N_TILES
        turn = idx // N_TILES
        branch = turn % 2
        layer = n_layers - 1 - turn // 2
        last = n_steps - N_TILES
        wide = (idx >= last - N_TILES) & (idx < last)
        narrow = idx < last - N_TILES

        def gather(waits, starts):
            for is_wide, cond in ((True, wide), (False, narrow)):
                @pl.when(cond)
                def _():
                    if waits is not None:
                        remote(waits, tile, is_wide).wait()
                    if starts is not None:
                        if is_wide:
                            pl.semaphore_wait(free_sem.at[tile, starts - 3], 1)
                        remote(starts, tile, is_wide).start()

        def release(slot, peer):
            @pl.when(wide)
            def _():
                pl.semaphore_signal(free_sem.at[tile, slot], inc=1, device_id={'tp': peer}, device_id_type=MESH)

        if stage == 'C':
            @pl.when(branch == 0)
            def _():
                mlp_tile(layer, tile)

            @pl.when(branch == 1)
            def _():
                attn_tile(layer, tile)
            remote(0, tile).start()
        elif stage == 'b':
            remote(0, tile).wait()
            release(2, mate)
            add_rows(tile, half, 64, rec_d)
            remote(1, tile).start()
        elif stage == 'c':
            remote(1, tile).wait()
            release(1, peer_one)
            add_rows(tile, quarter, 32, rec_one)
            remote(2, tile).start()
        elif stage == 'd':
            remote(2, tile).wait()
            release(0, peer_two)

            @pl.when(turn == 0)
            def _():
                for copy in own_loads(tile):
                    copy.wait()
            finish_rows(branch, tile, wide)
            gather(None, 3)
        elif stage == 'e':
            gather(3, 4)
        elif stage == 'f':
            gather(4, 5)
        else:
            gather(5, None)

    max_lag = max(lag for _, lag in ORDER)

    @pl.loop(0, n_steps + max_lag)
    def _(step):
        for stage, lag in ORDER:
            @pl.when((step >= lag) & (step < n_steps + lag))
            def _():
                run_stage(stage, step - lag)

    finals = [pltpu.make_async_copy(x_st.at[0], o_x1, out_sem.at[0]),
              pltpu.make_async_copy(d_st.at[1], o_dx2, out_sem.at[1])]
    for copy in finals:
        copy.start()
    for copy in finals:
        copy.wait()


def run_stack(mask, y_one, y_two, dy_one, dy_two, w_query, w_key, w_value, w_out, w_up, w_down):
    n_layers, width, ff = w_up.shape
    qw = w_out.shape[1]
    kw = w_key.shape[3]
    tokens = y_one.shape[0]
    any_spec = pl.BlockSpec(memory_space=pl.ANY)
    out = lambda *shape: jax.ShapeDtypeStruct((n_layers, tokens) + shape, BF16)
    rows = jax.ShapeDtypeStruct((N_TILES, 16, width), F32)
    full = jax.ShapeDtypeStruct((tokens, width), F32)
    return pl.pallas_call(
        functools.partial(stack_kernel, n_layers, width, ff, qw, kw),
        out_shape=(rows, rows, full, full,
                   out(width), out(width), out(ff), out(ff), out(width), out(width),
                   out(qw), out(qw), out(kw), out(kw)),
        in_specs=[pl.BlockSpec(memory_space=pltpu.VMEM)] + [any_spec] * 10,
        out_specs=(any_spec,) * 14,
        scratch_shapes=[
            pltpu.VMEM((N_TILES, 2, TILE, width), BF16),
            pltpu.VMEM((N_TILES, 2, TILE, width), F32),
            pltpu.VMEM((N_TILES, 2, 64, width), F32),
            pltpu.VMEM((N_TILES, 2, 32, width), F32),
            pltpu.VMEM((N_TILES, 2, 16, width), F32),
            pltpu.VMEM((2, N_TILES, 16, width), F32),
            pltpu.VMEM((2, N_TILES, 16, width), F32),
            pltpu.VMEM((width, ff), BF16),
            pltpu.VMEM((ff, width), BF16),
            pltpu.VMEM((width, qw + 2 * kw), BF16),
            pltpu.VMEM((qw, width), BF16),
            pltpu.VMEM((TILE, ff), BF16),
            pltpu.VMEM((TILE, ff), BF16),
            pltpu.VMEM((TILE, qw), BF16),
            pltpu.VMEM((TILE, qw + 2 * kw), BF16),
            pltpu.VMEM((TILE, qw + 2 * kw), BF16),
            pltpu.SemaphoreType.DMA((N_TILES, 6)),
            pltpu.SemaphoreType.DMA((N_TILES, 6)),
            pltpu.SemaphoreType.DMA((5 + qw // kw,)),
            pltpu.SemaphoreType.DMA((4, N_TILES)),
            pltpu.SemaphoreType.DMA((N_TILES, 2)),
            pltpu.SemaphoreType.DMA((8,)),
            pltpu.SemaphoreType.REGULAR((N_TILES, 3)),
        ],
        compiler_params=pltpu.CompilerParams(
            collective_id=0, has_side_effects=True, vmem_limit_bytes=67043328),
        name='stack',
    )(mask, y_one, y_two, dy_one, dy_two, w_query, w_key, w_value, w_out, w_up, w_down)


def order_rows(blocks):
    n_dev, n_tiles, n_rows, width = blocks.shape

    def source(pos):
        core, first, second = pos // 4, (pos // 2) % 2, pos % 2
        return core + (1 - core) * (4 * second + 2 * first) + core * (4 * first + 2 * second)

    def body(src, dst):
        for tile in range(n_tiles):
            dst[tile, 0] = src[0, tile]

    return pl.pallas_call(
        body,
        grid=(n_dev,),
        out_shape=jax.ShapeDtypeStruct((n_tiles, n_dev, n_rows, width), blocks.dtype),
        in_specs=[pl.BlockSpec((1, n_tiles, n_rows, width), lambda pos: (source(pos), 0, 0, 0))],
        out_specs=pl.BlockSpec((n_tiles, 1, n_rows, width), lambda pos: (0, pos, 0, 0)),
        cost_estimate=pl.CostEstimate(flops=10 ** 8, bytes_accessed=2 * blocks.size * 4, transcendentals=0),
        name='order_rows',
    )(blocks)


def tile_mask(seq_lens, seq_len):
    n_seq = TILE // seq_len
    row = lax.broadcasted_iota(jnp.int32, (N_TILES, TILE, TILE), 1)
    col = lax.broadcasted_iota(jnp.int32, (N_TILES, TILE, TILE), 2)
    lens = jnp.repeat(seq_lens.reshape(N_TILES, 1, n_seq), seq_len, axis=2)
    seen = (row // seq_len == col // seq_len) & (col <= row) & (col % seq_len < lens)
    return seen.astype(F32)


def solution(mesh):
    act_spec = P('dp', None, None)
    w_specs = (P(None, None, 'tp', None), P(None, None, 'tp', None), P(None, None, 'tp', None),
               P(None, 'tp', None, None), P(None, None, 'tp'), P(None, 'tp', None))
    g_specs = (P('dp', None, 'tp', None), P('dp', None, 'tp', None), P('dp', None, 'tp', None),
               P('dp', 'tp', None, None), P('dp', None, 'tp'), P('dp', 'tp', None))

    def local_fn(y_one, y_two, dy_one, dy_two, seq_lens, w_query, w_key, w_value, w_out, w_up, w_down):
        n_batch, seq_len, width = y_one.shape
        tokens = n_batch * seq_len
        n_layers, _, n_heads, head_dim = w_query.shape
        slots = w_key.shape[2]
        flat = lambda val: val.reshape(tokens, width)
        by_head = lambda val: jnp.transpose(val, (0, 2, 1, 3))
        x_one, dx_two, x_two, dx_one, n_g, e_g, h_all, u_all, n_f, e_f, a_all, dq, dk, dv = run_stack(
            tile_mask(seq_lens, seq_len), flat(y_one), flat(y_two), flat(dy_one), flat(dy_two),
            by_head(w_query), by_head(w_key), by_head(w_value),
            w_out.reshape(n_layers, n_heads * head_dim, width), w_up, w_down)
        shape = lambda val: val.reshape(n_batch, seq_len, width)
        whole = lambda val: shape(order_rows(lax.all_gather(val, 'tp', axis=0)))
        finals = (whole(x_one), shape(x_two), shape(dx_one), whole(dx_two))
        heads = lambda val, count: val.reshape(n_layers, tokens, count, head_dim)
        dot = functools.partial(jnp.einsum, preferred_element_type=F32)
        dw_query = dot('ltd,lthe->ldhe', n_f, heads(dq, n_heads))
        dw_key = dot('ltd,lthe->ldhe', n_f, heads(dk, slots))
        dw_value = dot('ltd,lthe->ldhe', n_f, heads(dv, slots))
        dw_out = dot('lthe,ltd->lhed', heads(a_all, n_heads), e_f)
        dw_up = dot('ltd,ltf->ldf', n_g, u_all)
        dw_down = dot('ltf,ltd->lfd', h_all, e_g)
        return finals + (dw_query, dw_key, dw_value, dw_out, dw_up, dw_down)

    return jax.shard_map(local_fn, mesh=mesh,
                         in_specs=(act_spec,) * 4 + (P('dp'),) + w_specs,
                         out_specs=(act_spec,) * 4 + g_specs,
                         check_vma=False)
```

```python
import functools

import jax
import jax.numpy as jnp
from jax import lax
from jax.experimental import pallas as pl
from jax.experimental.pallas import tpu as pltpu
from jax.sharding import PartitionSpec as P

F32 = jnp.float32
BF16 = jnp.bfloat16
EPS = 1e-5
MASK_VALUE = -1e30
MESH = pl.DeviceIdType.MESH
TILE = 128
N_TILES = 4
GELU_C = 0.7978845608028654
GELU_A = 0.044715
BOTH = (0, 1)
ORDER = (('e', BOTH, 3), ('b', (1,), 1), ('g', BOTH, 4), ('C', BOTH, 0), ('f', BOTH, 3), ('d', BOTH, 2),
         ('c', (0,), 1), ('b', (0,), 0), ('c', (1,), 1))


def dot_nn(lhs, rhs):
    return lax.dot_general(lhs, rhs, (((1,), (0,)), ((), ())), preferred_element_type=F32)


def dot_nt(lhs, rhs):
    return lax.dot_general(lhs, rhs, (((1,), (1,)), ((), ())), preferred_element_type=F32)


def dot_tn(lhs, rhs):
    return lax.dot_general(lhs, rhs, (((0,), (0,)), ((), ())), preferred_element_type=F32)


def inv_rms_of(x_val):
    return lax.rsqrt(jnp.mean(x_val * x_val, axis=-1, keepdims=True) + EPS)


def stack_kernel(n_layers, width, ff, qw, kw,
                 mask, y_one, y_two, dy_one, dy_two, w_query, w_key, w_value, w_out, w_up, w_down,
                 o_own, o_x2, o_dy1, o_ng, o_eg, o_h, o_u, o_nf, o_ef, o_a, o_dqkv,
                 ne, part, rec_d, rec_one, rec_two, x_st, d_st, wu, wd, wqkv, wo, h_buf, u_buf,
                 a_buf, dqkv_buf, q_buf, n_turn, h_turn, a_turn, send_sem, recv_sem, w_sem, in_sem, act_sem, out_sem, free_sem):
    n_steps = 2 * n_layers * N_TILES
    me = lax.axis_index('tp')
    core = me % 2
    x_pos = (me // 2) % 2
    y_pos = me // 4
    mate = me + 1 - 2 * core
    x_peer = me + 2 - 4 * x_pos
    y_peer = me + 4 - 8 * y_pos
    peer_one = x_peer * (1 - core) + y_peer * core
    peer_two = y_peer * (1 - core) + x_peer * core
    bit_one = x_pos * (1 - core) + y_pos * core
    bit_two = y_pos * (1 - core) + x_pos * core
    half = pl.multiple_of(core * 64, 64)
    half_other = pl.multiple_of(64 - core * 64, 64)
    quarter = pl.multiple_of(half + bit_one * 32, 32)
    quarter_other = pl.multiple_of(half + 32 - bit_one * 32, 32)
    own = pl.multiple_of(quarter + bit_two * 16, 16)
    own_other = pl.multiple_of(quarter + 16 - bit_two * 16, 16)

    def mlp_loads(layer):
        return (pltpu.make_async_copy(w_up.at[layer], wu, w_sem.at[0]),
                pltpu.make_async_copy(w_down.at[layer], wd, w_sem.at[1]))

    def attn_loads(layer):
        heads = [w_query.at[layer, head] for head in range(qw // kw)]
        heads += [w_key.at[layer, 0], w_value.at[layer, 0]]
        copies = [pltpu.make_async_copy(src, wqkv.at[:, pl.ds(pos * kw, kw)], w_sem.at[3 + pos])
                  for pos, src in enumerate(heads)]
        return copies + [pltpu.make_async_copy(w_out.at[layer], wo, w_sem.at[2])]

    def act_loads(tile):
        rows = pl.ds(tile * TILE, TILE)
        return (pltpu.make_async_copy(y_one.at[rows, :], part.at[tile, 0], act_sem.at[tile, 0]),
                pltpu.make_async_copy(dy_two.at[rows, :], part.at[tile, 1], act_sem.at[tile, 1]))

    def own_loads(tile):
        pairs = ((y_one, x_st.at[0]), (y_two, x_st.at[1]), (dy_one, d_st.at[0]), (dy_two, d_st.at[1]))
        return [pltpu.make_async_copy(src.at[pl.ds(tile * TILE + own, 16), :], dst.at[tile], in_sem.at[pos, tile])
                for pos, (src, dst) in enumerate(pairs)]

    for copy in act_loads(0):
        copy.start()
    for copy in mlp_loads(n_layers - 1):
        copy.start()
    for tile in range(1, N_TILES):
        for copy in act_loads(tile):
            copy.start()
    for tile in range(N_TILES):
        for copy in own_loads(tile):
            copy.start()
    for copy in attn_loads(n_layers - 1):
        copy.start()

    barrier = pltpu.get_barrier_semaphore()
    for peer in (mate, x_peer, y_peer):
        pl.semaphore_signal(barrier, inc=1, device_id={'tp': peer}, device_id_type=MESH)
    pl.semaphore_wait(barrier, 3)

    def copy_to(src, dst, tile, pos, peer):
        return pltpu.make_async_remote_copy(
            src_ref=src, dst_ref=dst, send_sem=send_sem.at[tile, pos], recv_sem=recv_sem.at[tile, pos],
            device_id={'tp': peer}, device_id_type=MESH)

    def scatter(stage, tile, unit):
        base, n_rows, dst, peer = ((half_other, 64, rec_d, mate), (quarter_other, 32, rec_one, peer_one),
                                   (own_other, 16, rec_two, peer_two))[stage]
        return copy_to(part.at[tile, unit, pl.ds(base, n_rows), :], dst.at[tile, unit], tile, 2 * stage + unit, peer)

    def spread(stage, tile, wide):
        base, n_rows, peer = ((own, 16, peer_two), (quarter, 32, peer_one), (half, 64, mate))[stage]
        ref = (part if wide else ne).at[tile, :, pl.ds(base, n_rows), :]
        return copy_to(ref, ref, tile, 6 + stage, peer)

    def convert(tile):
        @pl.loop(0, TILE // 16)
        def _(pos):
            rows = pl.ds(pl.multiple_of(pos * 16, 16), 16)
            x_val = part[tile, 0, rows, :]
            ne[tile, 0, rows, :] = (x_val * inv_rms_of(x_val)).astype(BF16)
            ne[tile, 1, rows, :] = part[tile, 1, rows, :].astype(BF16)

    def turn_rows(tile):
        @pl.loop(0, width // 256)
        def _(pos):
            cols = pl.ds(pl.multiple_of(pos * 256, 256), 256)
            n_turn[cols, :] = ne[tile, 0, :, cols].T

    def mlp_tile(layer, tile):
        @pl.when(layer == n_layers - 1)
        def _():
            for copy in act_loads(tile):
                copy.wait()
            convert(tile)


        rows = pl.ds(tile * TILE, TILE)
        saves = [pltpu.make_async_copy(n_turn, o_ng.at[layer, :, rows], out_sem.at[0]),
                 pltpu.make_async_copy(ne.at[tile, 1], o_eg.at[layer, rows, :], out_sem.at[1])]
        turn_rows(tile)
        for copy in saves:
            copy.start()

        @pl.when(tile == 0)
        def _():
            for copy in mlp_loads(layer):
                copy.wait()

        @pl.loop(0, ff // 256)
        def _(pos):
            cols = pl.ds(pl.multiple_of(pos * 256, 256), 256)
            pre = dot_nn(ne[tile, 0], wu[:, cols])
            d_act = dot_nt(ne[tile, 1], wd[cols, :])
            tanh_val = jnp.tanh(GELU_C * (pre + GELU_A * (pre * pre * pre)))
            act = (0.5 * pre * (1.0 + tanh_val)).astype(BF16)
            h_buf[:, cols] = act
            h_turn[cols, :] = act.T
            slope = 0.5 * (1.0 + tanh_val) + (0.5 * GELU_C) * pre * (1.0 - tanh_val * tanh_val) * (1.0 + (3.0 * GELU_A) * (pre * pre))
            u_buf[:, cols] = (slope * d_act).astype(BF16)

        more = [pltpu.make_async_copy(h_turn, o_h.at[layer, :, rows], out_sem.at[2]),
                pltpu.make_async_copy(u_buf, o_u.at[layer, rows, :], out_sem.at[3])]
        for copy in more:
            copy.start()

        @pl.loop(0, width // 512)
        def _(pos):
            cols = pl.ds(pl.multiple_of(pos * 512, 512), 512)
            part[tile, 0, :, cols] = dot_nn(h_buf[...], wd[:, cols])
        for copy in saves:
            copy.wait()
        scatter(0, tile, 0).start()

        @pl.loop(0, width // 512)
        def _(pos):
            cols = pl.ds(pl.multiple_of(pos * 512, 512), 512)
            part[tile, 1, :, cols] = dot_nt(u_buf[...], wu[cols, :])
        scatter(0, tile, 1).start()

        for copy in more:
            copy.wait()

        @pl.when((tile == N_TILES - 1) & (layer > 0))
        def _():
            for copy in mlp_loads(layer - 1):
                copy.start()

    def attn_tile(layer, tile):
        rows = pl.ds(tile * TILE, TILE)
        wide_saves = [pltpu.make_async_copy(part.at[tile, 0], o_x2.at[rows, :], out_sem.at[6]),
                      pltpu.make_async_copy(part.at[tile, 1], o_dy1.at[rows, :], out_sem.at[7])]

        @pl.when(layer == 0)
        def _():
            for copy in wide_saves:
                copy.start()
            convert(tile)

        saves = [pltpu.make_async_copy(n_turn, o_nf.at[layer, :, rows], out_sem.at[0]),
                 pltpu.make_async_copy(ne.at[tile, 1], o_ef.at[layer, rows, :], out_sem.at[1])]
        turn_rows(tile)
        for copy in saves:
            copy.start()

        @pl.when(tile == 0)
        def _():
            for copy in attn_loads(layer):
                copy.wait()

        n_val = ne[tile, 0]
        q_buf[:, :qw] = dot_nn(n_val, wqkv[:, :qw]).astype(BF16)
        q_buf[:, qw:] = dot_nn(n_val, wqkv[:, qw:]).astype(BF16)
        key = q_buf[:, qw:qw + kw]
        value = q_buf[:, qw + kw:]
        d_attn_all = dot_nt(ne[tile, 1], wo[...]).astype(BF16)
        visible = mask[tile] > 0.5
        scale = kw ** -0.5
        d_key = jnp.zeros((TILE, kw), F32)
        d_value = jnp.zeros((TILE, kw), F32)
        for head in range(qw // kw):
            cols = slice(head * kw, (head + 1) * kw)
            query = q_buf[:, cols]
            d_attn = d_attn_all[:, cols]
            scores = jnp.where(visible, dot_nt(query, key) * scale, MASK_VALUE)
            weights = jnp.exp(scores - jnp.max(scores, axis=-1, keepdims=True))
            probs = weights / jnp.sum(weights, axis=-1, keepdims=True)
            probs_b = probs.astype(BF16)
            mixed = dot_nn(probs_b, value).astype(BF16)
            a_buf[:, cols] = mixed
            a_turn[cols, :] = mixed.T
            d_value += dot_tn(probs_b, d_attn)
            d_probs = dot_nt(d_attn, value)
            d_scores = (probs * (d_probs - jnp.sum(d_probs * probs, axis=-1, keepdims=True)) * scale).astype(BF16)
            dqkv_buf[:, cols] = dot_nn(d_scores, key).astype(BF16)
            d_key += dot_tn(d_scores, query)
        dqkv_buf[:, qw:qw + kw] = d_key.astype(BF16)
        dqkv_buf[:, qw + kw:] = d_value.astype(BF16)

        more = [pltpu.make_async_copy(a_turn, o_a.at[layer, :, rows], out_sem.at[2]),
                pltpu.make_async_copy(dqkv_buf, o_dqkv.at[layer, rows, :], out_sem.at[3])]
        for copy in more:
            copy.start()

        @pl.when(layer == 0)
        def _():
            for copy in wide_saves:
                copy.wait()

        @pl.loop(0, width // 512)
        def _(pos):
            cols = pl.ds(pl.multiple_of(pos * 512, 512), 512)
            part[tile, 0, :, cols] = dot_nn(a_buf[...], wo[:, cols])
        for copy in saves:
            copy.wait()
        scatter(0, tile, 0).start()

        @pl.loop(0, width // 512)
        def _(pos):
            cols = pl.ds(pl.multiple_of(pos * 512, 512), 512)
            part[tile, 1, :, cols] = dot_nt(dqkv_buf[...], wqkv[cols, :])
        scatter(0, tile, 1).start()

        for copy in more:
            copy.wait()

        @pl.when((tile == N_TILES - 1) & (layer > 0))
        def _():
            for copy in attn_loads(layer - 1):
                copy.start()

    def add_rows(tile, unit, base, n_rows, received):
        @pl.loop(0, n_rows // 8)
        def _(pos):
            row = pl.multiple_of(pos * 8, 8)
            dst = pl.ds(pl.multiple_of(base + row, 8), 8)
            part[tile, unit, dst, :] += received[tile, unit, pl.ds(row, 8), :]

    def finish_rows(branch, tile, wide):
        rows = pl.ds(own, 16)
        other = 1 - branch
        x_new = x_st[other, tile] - (part[tile, 0, rows, :] + rec_two[tile, 0])
        x_st[other, tile] = x_new
        grad = part[tile, 1, rows, :] + rec_two[tile, 1]
        x_val = x_st[branch, tile]
        inv = inv_rms_of(x_val)
        normed = x_val * inv
        d_new = d_st[branch, tile] + inv * (grad - normed * jnp.mean(grad * normed, axis=-1, keepdims=True))
        d_st[branch, tile] = d_new

        @pl.when(wide)
        def _():
            part[tile, 0, rows, :] = x_new
            part[tile, 1, rows, :] = d_new

        @pl.when(jnp.logical_not(wide))
        def _():
            ne[tile, 0, rows, :] = (x_new * inv_rms_of(x_new)).astype(BF16)
            ne[tile, 1, rows, :] = d_new.astype(BF16)

    def run_stage(stage, units, idx):
        tile = idx % N_TILES
        turn = idx // N_TILES
        branch = turn % 2
        layer = n_layers - 1 - turn // 2
        last = n_steps - N_TILES
        wide = (idx >= last - N_TILES) & (idx < last)
        narrow = idx < last - N_TILES

        def gather(waits, starts):
            for is_wide, cond in ((True, wide), (False, narrow)):
                @pl.when(cond)
                def _():
                    if waits is not None:
                        spread(waits, tile, is_wide).wait()
                    if starts is not None:
                        if is_wide:
                            pl.semaphore_wait(free_sem.at[tile, starts], 2)
                        spread(starts, tile, is_wide).start()

        def release(slot, peer):
            @pl.when(wide)
            def _():
                pl.semaphore_signal(free_sem.at[tile, slot], inc=1, device_id={'tp': peer}, device_id_type=MESH)

        if stage == 'C':
            @pl.when(branch == 0)
            def _():
                mlp_tile(layer, tile)

            @pl.when(branch == 1)
            def _():
                attn_tile(layer, tile)
        elif stage == 'b':
            for unit in units:
                scatter(0, tile, unit).wait()
                release(2, mate)
                add_rows(tile, unit, half, 64, rec_d)
                scatter(1, tile, unit).start()
        elif stage == 'c':
            for unit in units:
                scatter(1, tile, unit).wait()
                release(1, peer_one)
                add_rows(tile, unit, quarter, 32, rec_one)
                scatter(2, tile, unit).start()
        elif stage == 'd':
            for unit in units:
                scatter(2, tile, unit).wait()
                release(0, peer_two)

            @pl.when(turn == 0)
            def _():
                for copy in own_loads(tile):
                    copy.wait()
            finish_rows(branch, tile, wide)
            gather(None, 0)
        elif stage == 'e':
            gather(0, 1)
        elif stage == 'f':
            gather(1, 2)
        else:
            gather(2, None)

    max_lag = max(lag for _, _, lag in ORDER)

    @pl.loop(0, n_steps + max_lag)
    def _(step):
        for stage, units, lag in ORDER:
            @pl.when((step >= lag) & (step < n_steps + lag))
            def _():
                run_stage(stage, units, step - lag)

    finals = [pltpu.make_async_copy(x_st.at[0], o_own.at[0], out_sem.at[0]),
              pltpu.make_async_copy(d_st.at[1], o_own.at[1], out_sem.at[1])]
    for copy in finals:
        copy.start()
    for copy in finals:
        copy.wait()


def run_stack(mask, y_one, y_two, dy_one, dy_two, w_query, w_key, w_value, w_out, w_up, w_down):
    n_layers, width, ff = w_up.shape
    qw = w_out.shape[1]
    kw = w_key.shape[3]
    tokens = y_one.shape[0]
    any_spec = pl.BlockSpec(memory_space=pl.ANY)
    out = lambda *shape: jax.ShapeDtypeStruct((n_layers, tokens) + shape, BF16)
    turned = lambda size: jax.ShapeDtypeStruct((n_layers, size, tokens), BF16)
    rows = jax.ShapeDtypeStruct((2, N_TILES, 16, width), F32)
    full = jax.ShapeDtypeStruct((tokens, width), F32)
    return pl.pallas_call(
        functools.partial(stack_kernel, n_layers, width, ff, qw, kw),
        out_shape=(rows, full, full,
                   turned(width), out(width), turned(ff), out(ff), turned(width), out(width),
                   turned(qw), out(qw + 2 * kw)),
        in_specs=[pl.BlockSpec(memory_space=pltpu.VMEM)] + [any_spec] * 10,
        out_specs=(any_spec,) * 11,
        scratch_shapes=[
            pltpu.VMEM((N_TILES, 2, TILE, width), BF16),
            pltpu.VMEM((N_TILES, 2, TILE, width), F32),
            pltpu.VMEM((N_TILES, 2, 64, width), F32),
            pltpu.VMEM((N_TILES, 2, 32, width), F32),
            pltpu.VMEM((N_TILES, 2, 16, width), F32),
            pltpu.VMEM((2, N_TILES, 16, width), F32),
            pltpu.VMEM((2, N_TILES, 16, width), F32),
            pltpu.VMEM((width, ff), BF16),
            pltpu.VMEM((ff, width), BF16),
            pltpu.VMEM((width, qw + 2 * kw), BF16),
            pltpu.VMEM((qw, width), BF16),
            pltpu.VMEM((TILE, ff), BF16),
            pltpu.VMEM((TILE, ff), BF16),
            pltpu.VMEM((TILE, qw), BF16),
            pltpu.VMEM((TILE, qw + 2 * kw), BF16),
            pltpu.VMEM((TILE, qw + 2 * kw), BF16),
            pltpu.VMEM((width, TILE), BF16),
            pltpu.VMEM((ff, TILE), BF16),
            pltpu.VMEM((qw, TILE), BF16),
            pltpu.SemaphoreType.DMA((N_TILES, 9)),
            pltpu.SemaphoreType.DMA((N_TILES, 9)),
            pltpu.SemaphoreType.DMA((5 + qw // kw,)),
            pltpu.SemaphoreType.DMA((4, N_TILES)),
            pltpu.SemaphoreType.DMA((N_TILES, 2)),
            pltpu.SemaphoreType.DMA((8,)),
            pltpu.SemaphoreType.REGULAR((N_TILES, 3)),
        ],
        compiler_params=pltpu.CompilerParams(
            collective_id=0, has_side_effects=True, vmem_limit_bytes=67043328),
        name='stack',
    )(mask, y_one, y_two, dy_one, dy_two, w_query, w_key, w_value, w_out, w_up, w_down)


def peers_of(index):
    core, x_pos, y_pos = index % 2, (index // 2) % 2, index // 4
    x_peer, y_peer = index + 2 - 4 * x_pos, index + 4 - 8 * y_pos
    return (x_peer if core else y_peer), (y_peer if core else x_peer), index + 1 - 2 * core


def slots_of_pieces():
    me = lax.axis_index('tp')
    core, x_pos, y_pos = me % 2, (me // 2) % 2, me // 4
    bit_one = x_pos * (1 - core) + y_pos * core
    bit_two = y_pos * (1 - core) + x_pos * core
    slots = []
    for side, first, second in ((core, bit_one, bit_two), (1 - core, bit_two, bit_one)):
        for flip_one, flip_two in ((0, 0), (0, 1), (1, 0), (1, 1)):
            one = first + flip_one - 2 * flip_one * first
            two = second + flip_two - 2 * flip_two * second
            slots.append(4 * side + 2 * one + two)
    return slots


def assemble(pieces):
    n_arrays, n_tiles, n_rows, width = pieces[0].shape
    n_pieces = len(pieces)
    shape = jax.ShapeDtypeStruct((n_tiles, n_pieces, n_rows, width), F32)

    def body(*refs):
        outs, out_sem = refs[n_pieces:-1], refs[-1]
        copies = [pltpu.make_async_copy(refs[pos].at[which], out.at[:, slot], out_sem.at[pos, which])
                  for pos, slot in enumerate(slots_of_pieces()) for which, out in enumerate(outs)]
        for copy in copies:
            copy.start()
        for copy in copies:
            copy.wait()

    return pl.pallas_call(
        body,
        out_shape=(shape,) * n_arrays,
        in_specs=[pl.BlockSpec(memory_space=pltpu.VMEM)] * n_pieces,
        out_specs=(pl.BlockSpec(memory_space=pl.ANY),) * n_arrays,
        scratch_shapes=[pltpu.SemaphoreType.DMA((n_pieces, n_arrays))],
        compiler_params=pltpu.CompilerParams(vmem_limit_bytes=32 * 2 ** 20),
        name='assemble',
    )(*pieces)


def copy_out(arrays):
    n_parts = 4
    n_rows, width = arrays[0].shape
    size = n_rows // n_parts
    count = len(arrays) * n_parts

    def body(*refs):
        srcs, dsts = refs[:len(arrays)], refs[len(arrays):2 * len(arrays)]
        buf, in_sem, out_sem = refs[2 * len(arrays):]
        rows = lambda pos: pl.ds((pos % n_parts) * size, size)
        loads = [pltpu.make_async_copy(srcs[pos // n_parts].at[rows(pos), :], buf.at[pos], in_sem.at[pos]) for pos in range(count)]
        stores = [pltpu.make_async_copy(buf.at[pos], dsts[pos // n_parts].at[rows(pos), :], out_sem.at[pos]) for pos in range(count)]
        for copy in loads:
            copy.start()
        for load, store in zip(loads, stores):
            load.wait()
            store.start()
        for copy in stores:
            copy.wait()

    any_spec = pl.BlockSpec(memory_space=pl.ANY)
    return pl.pallas_call(
        body,
        out_shape=tuple(jax.ShapeDtypeStruct(arr.shape, arr.dtype) for arr in arrays),
        in_specs=[any_spec] * len(arrays),
        out_specs=(any_spec,) * len(arrays),
        scratch_shapes=[pltpu.VMEM((count, size, width), F32),
                        pltpu.SemaphoreType.DMA((count,)), pltpu.SemaphoreType.DMA((count,))],
        compiler_params=pltpu.CompilerParams(vmem_limit_bytes=32 * 2 ** 20),
        name='copy_out',
    )(*arrays)


def layer_dot(lhs, rhs, block, splits):
    n_layers, n_rows, tokens = lhs.shape
    cols = rhs.shape[2]
    per_layer = n_rows // block
    total = n_layers * per_layer
    n_out, n_in = 4, 3
    n_heads = sum(splits) if splits else 1
    head = cols // n_heads

    def body(lhs_ref, rhs_ref, *refs):
        outs = refs[:-6]
        lhs_buf, rhs_buf, out_buf, lhs_sem, rhs_sem, out_sem = refs[-6:]

        def rows(step):
            return pl.ds(pl.multiple_of((step % per_layer) * block, block), block)

        def lhs_load(step):
            return pltpu.make_async_copy(lhs_ref.at[step // per_layer, rows(step), :], lhs_buf.at[step % n_in], lhs_sem.at[step % n_in])

        def rhs_load(layer):
            return pltpu.make_async_copy(rhs_ref.at[layer], rhs_buf.at[layer], rhs_sem.at[layer])

        def stores(step):
            slot, layer = step % n_out, step // per_layer
            if not splits:
                return [pltpu.make_async_copy(out_buf.at[slot], outs[0].at[layer, rows(step), :], out_sem.at[slot, 0])]
            places = [(out, pos) for out, count in zip(outs, splits) for pos in range(count)]
            return [pltpu.make_async_copy(out_buf.at[slot, :, pl.ds(num * head, head)], out.at[layer, pos, rows(step), :], out_sem.at[slot, num])
                    for num, (out, pos) in enumerate(places)]

        rhs_load(0).start()
        for step in range(n_in - 1):
            lhs_load(step).start()
        for layer in range(1, n_layers):
            rhs_load(layer).start()

        @pl.loop(0, total)
        def _(step):
            @pl.when(step % per_layer == 0)
            def _():
                rhs_load(step // per_layer).wait()
            lhs_load(step).wait()

            @pl.when(step + n_in - 1 < total)
            def _():
                lhs_load(step + n_in - 1).start()

            @pl.when(step >= n_out)
            def _():
                for copy in stores(step - n_out):
                    copy.wait()
            out_buf[step % n_out] = dot_nn(lhs_buf[step % n_in], rhs_buf[step // per_layer])
            for copy in stores(step):
                copy.start()

        for step in range(total - n_out, total):
            for copy in stores(step):
                copy.wait()

    if splits:
        out_shape = tuple(jax.ShapeDtypeStruct((n_layers, count, n_rows, head), F32) for count in splits)
    else:
        out_shape = (jax.ShapeDtypeStruct((n_layers, n_rows, cols), F32),)
    any_spec = pl.BlockSpec(memory_space=pl.ANY)
    return pl.pallas_call(
        body,
        out_shape=out_shape,
        in_specs=[any_spec, any_spec],
        out_specs=(any_spec,) * len(out_shape),
        scratch_shapes=[pltpu.VMEM((n_in, block, tokens), BF16),
                        pltpu.VMEM((n_layers, tokens, cols), BF16),
                        pltpu.VMEM((n_out, block, cols), F32),
                        pltpu.SemaphoreType.DMA((n_in,)),
                        pltpu.SemaphoreType.DMA((n_layers,)),
                        pltpu.SemaphoreType.DMA((n_out, n_heads))],
        compiler_params=pltpu.CompilerParams(vmem_limit_bytes=32 * 2 ** 20),
        cost_estimate=pl.CostEstimate(flops=2 * n_layers * n_rows * cols * tokens,
                                      bytes_accessed=4 * n_layers * n_rows * cols, transcendentals=0),
        name='layer_dot',
    )(lhs, rhs)


def gather_rows(val, work):
    perms = [[(index, peers_of(index)[pos]) for index in range(8)] for pos in range(3)]
    send = lambda rows, pos: lax.ppermute(rows, 'tp', perms[pos])
    second, first, mate = send(val, 0), send(val, 1), send(val, 2)
    results = [work[0]()]
    second, first, results[0] = lax.optimization_barrier((second, first, results[0]))
    both, mate_second, mate_first = send(second, 1), send(second, 2), send(first, 2)
    results.append(work[1]())
    both, results[1] = lax.optimization_barrier((both, results[1]))
    mate_both = send(both, 2)
    results.append(work[2]())
    mate_both, results[2] = lax.optimization_barrier((mate_both, results[2]))
    return assemble([val, second, first, both, mate, mate_second, mate_first, mate_both]), results


def tile_mask(seq_lens, seq_len):
    n_seq = TILE // seq_len
    row = lax.broadcasted_iota(jnp.int32, (N_TILES, TILE, TILE), 1)
    col = lax.broadcasted_iota(jnp.int32, (N_TILES, TILE, TILE), 2)
    lens = jnp.repeat(seq_lens.reshape(N_TILES, 1, n_seq), seq_len, axis=2)
    seen = (row // seq_len == col // seq_len) & (col <= row) & (col % seq_len < lens)
    return seen.astype(F32)


def solution(mesh):
    act_spec = P('dp', None, None)
    w_specs = (P(None, None, 'tp', None), P(None, None, 'tp', None), P(None, None, 'tp', None),
               P(None, 'tp', None, None), P(None, None, 'tp'), P(None, 'tp', None))
    g_specs = (P('dp', None, 'tp', None), P('dp', None, 'tp', None), P('dp', None, 'tp', None),
               P('dp', 'tp', None, None), P('dp', None, 'tp'), P('dp', 'tp', None))

    def local_fn(y_one, y_two, dy_one, dy_two, seq_lens, w_query, w_key, w_value, w_out, w_up, w_down):
        n_batch, seq_len, width = y_one.shape
        tokens = n_batch * seq_len
        n_layers, _, n_heads, head_dim = w_query.shape
        slots = w_key.shape[2]
        flat = lambda val: val.reshape(tokens, width)
        by_head = lambda val: jnp.transpose(val, (0, 2, 1, 3))
        own_rows, x_two, dx_one, n_g, e_g, h_all, u_all, n_f, e_f, a_all, dqkv = run_stack(
            tile_mask(seq_lens, seq_len), flat(y_one), flat(y_two), flat(dy_one), flat(dy_two),
            by_head(w_query), by_head(w_key), by_head(w_value),
            w_out.reshape(n_layers, n_heads * head_dim, width), w_up, w_down)
        shape = lambda val: val.reshape(n_batch, seq_len, width)
        (x_one, dx_two), (mlp_grads, attn_grads, copies) = gather_rows(own_rows, (
            lambda: layer_dot(n_g, u_all, 512, ()) + layer_dot(h_all, e_g, 256, ()),
            lambda: layer_dot(n_f, dqkv, 512, (n_heads, slots, slots)) + layer_dot(a_all, e_f, 128, ()),
            lambda: copy_out([x_two, dx_one])))
        finals = tuple(shape(val) for val in (x_one, copies[0], copies[1], dx_two))
        dw_up, dw_down = mlp_grads
        dw_query, dw_key, dw_value = (by_head(val) for val in attn_grads[:3])
        dw_out = attn_grads[3].reshape(n_layers, n_heads, head_dim, width)
        return finals + (dw_query, dw_key, dw_value, dw_out, dw_up, dw_down)

    return jax.shard_map(local_fn, mesh=mesh,
                         in_specs=(act_spec,) * 4 + (P('dp'),) + w_specs,
                         out_specs=(act_spec,) * 4 + g_specs,
                         check_vma=False)
```

```python
import functools

import jax
import jax.numpy as jnp
from jax import lax
from jax.experimental import pallas as pl
from jax.experimental.pallas import tpu as pltpu
from jax.sharding import PartitionSpec as P

F32 = jnp.float32
BF16 = jnp.bfloat16
EPS = 1e-5
MASK_VALUE = -1e30
MESH = pl.DeviceIdType.MESH
TILE = 128
N_TILES = 4
GELU_C = 0.7978845608028654
GELU_A = 0.044715
BOTH = (0, 1)
ORDER = (('e', BOTH, 3), ('b', (1,), 1), ('g', BOTH, 4), ('C', BOTH, 0), ('f', BOTH, 3), ('d', BOTH, 2),
         ('c', (0,), 1), ('b', (0,), 0), ('c', (1,), 1))


def dot_nn(lhs, rhs):
    return lax.dot_general(lhs, rhs, (((1,), (0,)), ((), ())), preferred_element_type=F32)


def dot_nt(lhs, rhs):
    return lax.dot_general(lhs, rhs, (((1,), (1,)), ((), ())), preferred_element_type=F32)


def dot_tn(lhs, rhs):
    return lax.dot_general(lhs, rhs, (((0,), (0,)), ((), ())), preferred_element_type=F32)


def inv_rms_of(x_val):
    return lax.rsqrt(jnp.mean(x_val * x_val, axis=-1, keepdims=True) + EPS)


def stack_kernel(n_layers, width, ff, qw, kw, seq_len,
                 lens, y_one, y_two, dy_one, dy_two, w_query, w_key, w_value, w_out, w_up, w_down,
                 o_own, o_x2, o_dy1, o_ng, o_eg, o_h, o_u, o_nf, o_ef, o_a, o_dqkv,
                 ne, part, rec_d, rec_one, rec_two, x_st, d_st, wu, wd, wqkv, wo, h_buf, u_buf,
                 a_buf, dqkv_buf, q_buf, n_turn, h_turn, a_turn, send_sem, recv_sem, w_sem, in_sem, act_sem, out_sem, free_sem):
    n_steps = 2 * n_layers * N_TILES
    me = lax.axis_index('tp')
    core = me % 2
    x_pos = (me // 2) % 2
    y_pos = me // 4
    mate = me + 1 - 2 * core
    x_peer = me + 2 - 4 * x_pos
    y_peer = me + 4 - 8 * y_pos
    peer_one = x_peer * (1 - core) + y_peer * core
    peer_two = y_peer * (1 - core) + x_peer * core
    bit_one = x_pos * (1 - core) + y_pos * core
    bit_two = y_pos * (1 - core) + x_pos * core
    half = pl.multiple_of(core * 64, 64)
    half_other = pl.multiple_of(64 - core * 64, 64)
    quarter = pl.multiple_of(half + bit_one * 32, 32)
    quarter_other = pl.multiple_of(half + 32 - bit_one * 32, 32)
    own = pl.multiple_of(quarter + bit_two * 16, 16)
    own_other = pl.multiple_of(quarter + 16 - bit_two * 16, 16)

    def mlp_loads(layer):
        return (pltpu.make_async_copy(w_up.at[layer], wu, w_sem.at[0]),
                pltpu.make_async_copy(w_down.at[layer], wd, w_sem.at[1]))

    def attn_loads(layer):
        heads = [w_query.at[layer, head] for head in range(qw // kw)]
        heads += [w_key.at[layer, 0], w_value.at[layer, 0]]
        copies = [pltpu.make_async_copy(src, wqkv.at[:, pl.ds(pos * kw, kw)], w_sem.at[3 + pos])
                  for pos, src in enumerate(heads)]
        return copies + [pltpu.make_async_copy(w_out.at[layer], wo, w_sem.at[2])]

    def act_loads(tile):
        rows = pl.ds(tile * TILE, TILE)
        return (pltpu.make_async_copy(y_one.at[rows, :], part.at[tile, 0], act_sem.at[tile, 0]),
                pltpu.make_async_copy(dy_two.at[rows, :], part.at[tile, 1], act_sem.at[tile, 1]))

    def own_loads(tile):
        pairs = ((y_one, x_st.at[0]), (y_two, x_st.at[1]), (dy_one, d_st.at[0]), (dy_two, d_st.at[1]))
        return [pltpu.make_async_copy(src.at[pl.ds(tile * TILE + own, 16), :], dst.at[tile], in_sem.at[pos, tile])
                for pos, (src, dst) in enumerate(pairs)]

    for copy in act_loads(0):
        copy.start()
    for copy in mlp_loads(n_layers - 1):
        copy.start()
    for tile in range(1, N_TILES):
        for copy in act_loads(tile):
            copy.start()
    for tile in range(N_TILES):
        for copy in own_loads(tile):
            copy.start()
    for copy in attn_loads(n_layers - 1):
        copy.start()

    barrier = pltpu.get_barrier_semaphore()
    for peer in (mate, x_peer, y_peer):
        pl.semaphore_signal(barrier, inc=1, device_id={'tp': peer}, device_id_type=MESH)
    pl.semaphore_wait(barrier, 3)

    def copy_to(src, dst, tile, pos, peer):
        return pltpu.make_async_remote_copy(
            src_ref=src, dst_ref=dst, send_sem=send_sem.at[tile, pos], recv_sem=recv_sem.at[tile, pos],
            device_id={'tp': peer}, device_id_type=MESH)

    def scatter(stage, tile, unit):
        base, n_rows, dst, peer = ((half_other, 64, rec_d, mate), (quarter_other, 32, rec_one, peer_one),
                                   (own_other, 16, rec_two, peer_two))[stage]
        return copy_to(part.at[tile, unit, pl.ds(base, n_rows), :], dst.at[tile, unit], tile, 2 * stage + unit, peer)

    def spread(stage, tile, wide):
        base, n_rows, peer = ((own, 16, peer_two), (quarter, 32, peer_one), (half, 64, mate))[stage]
        ref = (part if wide else ne).at[tile, :, pl.ds(base, n_rows), :]
        return copy_to(ref, ref, tile, 6 + stage, peer)

    def convert(tile):
        @pl.loop(0, TILE // 16, unroll=2)
        def _(pos):
            rows = pl.ds(pl.multiple_of(pos * 16, 16), 16)
            x_val = part[tile, 0, rows, :]
            ne[tile, 0, rows, :] = (x_val * inv_rms_of(x_val)).astype(BF16)
            ne[tile, 1, rows, :] = part[tile, 1, rows, :].astype(BF16)

    def turn_rows(tile):
        @pl.loop(0, width // 256, unroll=4)
        def _(pos):
            cols = pl.ds(pl.multiple_of(pos * 256, 256), 256)
            n_turn[cols, :] = ne[tile, 0, :, cols].T

    def mlp_tile(layer, tile):
        @pl.when(layer == n_layers - 1)
        def _():
            for copy in act_loads(tile):
                copy.wait()
            convert(tile)


        rows = pl.ds(tile * TILE, TILE)
        saves = [pltpu.make_async_copy(n_turn, o_ng.at[layer, :, rows], out_sem.at[0]),
                 pltpu.make_async_copy(ne.at[tile, 1], o_eg.at[layer, rows, :], out_sem.at[1])]
        turn_rows(tile)
        for copy in saves:
            copy.start()

        @pl.when(tile == 0)
        def _():
            for copy in mlp_loads(layer):
                copy.wait()

        @pl.loop(0, ff // 256, unroll=True)
        def _(pos):
            cols = pl.ds(pl.multiple_of(pos * 256, 256), 256)
            pre = dot_nn(ne[tile, 0], wu[:, cols])
            d_act = dot_nt(ne[tile, 1], wd[cols, :])
            tanh_val = jnp.tanh(GELU_C * (pre + GELU_A * (pre * pre * pre)))
            act = (0.5 * pre * (1.0 + tanh_val)).astype(BF16)
            h_buf[:, cols] = act
            h_turn[cols, :] = act.T
            slope = 0.5 * (1.0 + tanh_val) + (0.5 * GELU_C) * pre * (1.0 - tanh_val * tanh_val) * (1.0 + (3.0 * GELU_A) * (pre * pre))
            u_buf[:, cols] = (slope * d_act).astype(BF16)

        more = [pltpu.make_async_copy(h_turn, o_h.at[layer, :, rows], out_sem.at[2]),
                pltpu.make_async_copy(u_buf, o_u.at[layer, rows, :], out_sem.at[3])]
        for copy in more:
            copy.start()

        @pl.loop(0, width // 512, unroll=True)
        def _(pos):
            cols = pl.ds(pl.multiple_of(pos * 512, 512), 512)
            part[tile, 0, :, cols] = dot_nn(h_buf[...], wd[:, cols])
        for copy in saves:
            copy.wait()
        scatter(0, tile, 0).start()

        @pl.loop(0, width // 512, unroll=True)
        def _(pos):
            cols = pl.ds(pl.multiple_of(pos * 512, 512), 512)
            part[tile, 1, :, cols] = dot_nt(u_buf[...], wu[cols, :])
        scatter(0, tile, 1).start()

        for copy in more:
            copy.wait()

        @pl.when((tile == N_TILES - 1) & (layer > 0))
        def _():
            for copy in mlp_loads(layer - 1):
                copy.start()

    def tile_mask(tile):
        row = lax.broadcasted_iota(jnp.int32, (TILE, TILE), 0)
        col = lax.broadcasted_iota(jnp.int32, (TILE, TILE), 1)
        seen = jnp.zeros((TILE, TILE), jnp.bool_)
        n_seq = TILE // seq_len
        for pos in range(n_seq):
            base = pos * seq_len
            inside = (row >= base) & (row < base + seq_len)
            seen = seen | (inside & (col >= base) & (col < base + lens[tile * n_seq + pos]))
        return seen & (col <= row)

    def attn_tile(layer, tile):
        rows = pl.ds(tile * TILE, TILE)
        wide_saves = [pltpu.make_async_copy(part.at[tile, 0], o_x2.at[rows, :], out_sem.at[6]),
                      pltpu.make_async_copy(part.at[tile, 1], o_dy1.at[rows, :], out_sem.at[7])]

        @pl.when(layer == 0)
        def _():
            for copy in wide_saves:
                copy.start()
            convert(tile)

        saves = [pltpu.make_async_copy(n_turn, o_nf.at[layer, :, rows], out_sem.at[0]),
                 pltpu.make_async_copy(ne.at[tile, 1], o_ef.at[layer, rows, :], out_sem.at[1])]
        turn_rows(tile)
        for copy in saves:
            copy.start()

        @pl.when(tile == 0)
        def _():
            for copy in attn_loads(layer):
                copy.wait()

        n_val = ne[tile, 0]
        q_buf[:, :qw] = dot_nn(n_val, wqkv[:, :qw]).astype(BF16)
        q_buf[:, qw:] = dot_nn(n_val, wqkv[:, qw:]).astype(BF16)
        key = q_buf[:, qw:qw + kw]
        value = q_buf[:, qw + kw:]
        d_attn_all = dot_nt(ne[tile, 1], wo[...]).astype(BF16)
        visible = tile_mask(tile)
        scale = kw ** -0.5
        d_key = jnp.zeros((TILE, kw), F32)
        d_value = jnp.zeros((TILE, kw), F32)
        for head in range(qw // kw):
            cols = slice(head * kw, (head + 1) * kw)
            query = q_buf[:, cols]
            d_attn = d_attn_all[:, cols]
            scores = jnp.where(visible, dot_nt(query, key) * scale, MASK_VALUE)
            weights = jnp.exp(scores - jnp.max(scores, axis=-1, keepdims=True))
            probs = weights / jnp.sum(weights, axis=-1, keepdims=True)
            probs_b = probs.astype(BF16)
            mixed = dot_nn(probs_b, value).astype(BF16)
            a_buf[:, cols] = mixed
            a_turn[cols, :] = mixed.T
            d_value += dot_tn(probs_b, d_attn)
            d_probs = dot_nt(d_attn, value)
            d_scores = (probs * (d_probs - jnp.sum(d_probs * probs, axis=-1, keepdims=True)) * scale).astype(BF16)
            dqkv_buf[:, cols] = dot_nn(d_scores, key).astype(BF16)
            d_key += dot_tn(d_scores, query)
        dqkv_buf[:, qw:qw + kw] = d_key.astype(BF16)
        dqkv_buf[:, qw + kw:] = d_value.astype(BF16)

        more = [pltpu.make_async_copy(a_turn, o_a.at[layer, :, rows], out_sem.at[2]),
                pltpu.make_async_copy(dqkv_buf, o_dqkv.at[layer, rows, :], out_sem.at[3])]
        for copy in more:
            copy.start()

        @pl.when(layer == 0)
        def _():
            for copy in wide_saves:
                copy.wait()

        @pl.loop(0, width // 512, unroll=True)
        def _(pos):
            cols = pl.ds(pl.multiple_of(pos * 512, 512), 512)
            part[tile, 0, :, cols] = dot_nn(a_buf[...], wo[:, cols])
        for copy in saves:
            copy.wait()
        scatter(0, tile, 0).start()

        @pl.loop(0, width // 512, unroll=True)
        def _(pos):
            cols = pl.ds(pl.multiple_of(pos * 512, 512), 512)
            part[tile, 1, :, cols] = dot_nt(dqkv_buf[...], wqkv[cols, :])
        scatter(0, tile, 1).start()

        for copy in more:
            copy.wait()

        @pl.when((tile == N_TILES - 1) & (layer > 0))
        def _():
            for copy in attn_loads(layer - 1):
                copy.start()

    def add_rows(tile, unit, base, n_rows, received):
        @pl.loop(0, n_rows // 8, unroll=2)
        def _(pos):
            row = pl.multiple_of(pos * 8, 8)
            dst = pl.ds(pl.multiple_of(base + row, 8), 8)
            part[tile, unit, dst, :] += received[tile, unit, pl.ds(row, 8), :]

    def finish_rows(branch, tile, wide):
        rows = pl.ds(own, 16)
        other = 1 - branch
        x_new = x_st[other, tile] - (part[tile, 0, rows, :] + rec_two[tile, 0])
        x_st[other, tile] = x_new
        grad = part[tile, 1, rows, :] + rec_two[tile, 1]
        x_val = x_st[branch, tile]
        inv = inv_rms_of(x_val)
        normed = x_val * inv
        d_new = d_st[branch, tile] + inv * (grad - normed * jnp.mean(grad * normed, axis=-1, keepdims=True))
        d_st[branch, tile] = d_new

        @pl.when(wide)
        def _():
            part[tile, 0, rows, :] = x_new
            part[tile, 1, rows, :] = d_new

        @pl.when(jnp.logical_not(wide))
        def _():
            ne[tile, 0, rows, :] = (x_new * inv_rms_of(x_new)).astype(BF16)
            ne[tile, 1, rows, :] = d_new.astype(BF16)

    def run_stage(stage, units, idx):
        tile = idx % N_TILES
        turn = idx // N_TILES
        branch = turn % 2
        layer = n_layers - 1 - turn // 2
        last = n_steps - N_TILES
        wide = (idx >= last - N_TILES) & (idx < last)
        narrow = idx < last - N_TILES

        def gather(waits, starts):
            for is_wide, cond in ((True, wide), (False, narrow)):
                @pl.when(cond)
                def _():
                    if waits is not None:
                        spread(waits, tile, is_wide).wait()
                    if starts is not None:
                        if is_wide:
                            pl.semaphore_wait(free_sem.at[tile, starts], 2)
                        spread(starts, tile, is_wide).start()

        def release(slot, peer):
            @pl.when(wide)
            def _():
                pl.semaphore_signal(free_sem.at[tile, slot], inc=1, device_id={'tp': peer}, device_id_type=MESH)

        if stage == 'C':
            @pl.when(branch == 0)
            def _():
                mlp_tile(layer, tile)

            @pl.when(branch == 1)
            def _():
                attn_tile(layer, tile)
        elif stage == 'b':
            for unit in units:
                scatter(0, tile, unit).wait()
                release(2, mate)
                add_rows(tile, unit, half, 64, rec_d)
                scatter(1, tile, unit).start()
        elif stage == 'c':
            for unit in units:
                scatter(1, tile, unit).wait()
                release(1, peer_one)
                add_rows(tile, unit, quarter, 32, rec_one)
                scatter(2, tile, unit).start()
        elif stage == 'd':
            for unit in units:
                scatter(2, tile, unit).wait()
                release(0, peer_two)

            @pl.when(turn == 0)
            def _():
                for copy in own_loads(tile):
                    copy.wait()
            finish_rows(branch, tile, wide)
            gather(None, 0)
        elif stage == 'e':
            gather(0, 1)
        elif stage == 'f':
            gather(1, 2)
        else:
            gather(2, None)

    max_lag = max(lag for _, _, lag in ORDER)

    @pl.loop(0, n_steps + max_lag)
    def _(step):
        for stage, units, lag in ORDER:
            @pl.when((step >= lag) & (step < n_steps + lag))
            def _():
                run_stage(stage, units, step - lag)

    finals = [pltpu.make_async_copy(x_st.at[0], o_own.at[0], out_sem.at[0]),
              pltpu.make_async_copy(d_st.at[1], o_own.at[1], out_sem.at[1])]
    for copy in finals:
        copy.start()
    for copy in finals:
        copy.wait()


def run_stack(seq_lens, y_one, y_two, dy_one, dy_two, w_query, w_key, w_value, w_out, w_up, w_down):
    n_layers, width, ff = w_up.shape
    qw = w_out.shape[1]
    kw = w_key.shape[3]
    tokens = y_one.shape[0]
    any_spec = pl.BlockSpec(memory_space=pl.ANY)
    out = lambda *shape: jax.ShapeDtypeStruct((n_layers, tokens) + shape, BF16)
    turned = lambda size: jax.ShapeDtypeStruct((n_layers, size, tokens), BF16)
    rows = jax.ShapeDtypeStruct((2, N_TILES, 16, width), F32)
    full = jax.ShapeDtypeStruct((tokens, width), F32)
    return pl.pallas_call(
        functools.partial(stack_kernel, n_layers, width, ff, qw, kw, tokens // seq_lens.shape[0]),
        out_shape=(rows, full, full,
                   turned(width), out(width), turned(ff), out(ff), turned(width), out(width),
                   turned(qw), out(qw + 2 * kw)),
        in_specs=[pl.BlockSpec(memory_space=pltpu.SMEM)] + [any_spec] * 10,
        out_specs=(any_spec,) * 11,
        scratch_shapes=[
            pltpu.VMEM((N_TILES, 2, TILE, width), BF16),
            pltpu.VMEM((N_TILES, 2, TILE, width), F32),
            pltpu.VMEM((N_TILES, 2, 64, width), F32),
            pltpu.VMEM((N_TILES, 2, 32, width), F32),
            pltpu.VMEM((N_TILES, 2, 16, width), F32),
            pltpu.VMEM((2, N_TILES, 16, width), F32),
            pltpu.VMEM((2, N_TILES, 16, width), F32),
            pltpu.VMEM((width, ff), BF16),
            pltpu.VMEM((ff, width), BF16),
            pltpu.VMEM((width, qw + 2 * kw), BF16),
            pltpu.VMEM((qw, width), BF16),
            pltpu.VMEM((TILE, ff), BF16),
            pltpu.VMEM((TILE, ff), BF16),
            pltpu.VMEM((TILE, qw), BF16),
            pltpu.VMEM((TILE, qw + 2 * kw), BF16),
            pltpu.VMEM((TILE, qw + 2 * kw), BF16),
            pltpu.VMEM((width, TILE), BF16),
            pltpu.VMEM((ff, TILE), BF16),
            pltpu.VMEM((qw, TILE), BF16),
            pltpu.SemaphoreType.DMA((N_TILES, 9)),
            pltpu.SemaphoreType.DMA((N_TILES, 9)),
            pltpu.SemaphoreType.DMA((5 + qw // kw,)),
            pltpu.SemaphoreType.DMA((4, N_TILES)),
            pltpu.SemaphoreType.DMA((N_TILES, 2)),
            pltpu.SemaphoreType.DMA((8,)),
            pltpu.SemaphoreType.REGULAR((N_TILES, 3)),
        ],
        compiler_params=pltpu.CompilerParams(
            collective_id=0, has_side_effects=True, vmem_limit_bytes=67043328),
        name='stack',
    )(seq_lens, y_one, y_two, dy_one, dy_two, w_query, w_key, w_value, w_out, w_up, w_down)


def peers_of(index):
    core, x_pos, y_pos = index % 2, (index // 2) % 2, index // 4
    x_peer, y_peer = index + 2 - 4 * x_pos, index + 4 - 8 * y_pos
    return (x_peer if core else y_peer), (y_peer if core else x_peer), index + 1 - 2 * core


def slots_of_pieces():
    me = lax.axis_index('tp')
    core, x_pos, y_pos = me % 2, (me // 2) % 2, me // 4
    bit_one = x_pos * (1 - core) + y_pos * core
    bit_two = y_pos * (1 - core) + x_pos * core
    slots = []
    for side, first, second in ((core, bit_one, bit_two), (1 - core, bit_two, bit_one)):
        for flip_one, flip_two in ((0, 0), (0, 1), (1, 0), (1, 1)):
            one = first + flip_one - 2 * flip_one * first
            two = second + flip_two - 2 * flip_two * second
            slots.append(4 * side + 2 * one + two)
    return slots


def assemble(pieces):
    n_arrays, n_tiles, n_rows, width = pieces[0].shape
    n_pieces = len(pieces)
    shape = jax.ShapeDtypeStruct((n_tiles, n_pieces, n_rows, width), F32)

    def body(*refs):
        outs, out_sem = refs[n_pieces:-1], refs[-1]
        copies = [pltpu.make_async_copy(refs[pos].at[which], out.at[:, slot], out_sem.at[pos, which])
                  for pos, slot in enumerate(slots_of_pieces()) for which, out in enumerate(outs)]
        for copy in copies:
            copy.start()
        for copy in copies:
            copy.wait()

    return pl.pallas_call(
        body,
        out_shape=(shape,) * n_arrays,
        in_specs=[pl.BlockSpec(memory_space=pltpu.VMEM)] * n_pieces,
        out_specs=(pl.BlockSpec(memory_space=pl.ANY),) * n_arrays,
        scratch_shapes=[pltpu.SemaphoreType.DMA((n_pieces, n_arrays))],
        compiler_params=pltpu.CompilerParams(vmem_limit_bytes=32 * 2 ** 20),
        name='assemble',
    )(*pieces)


def copy_out(arrays):
    n_parts = 4
    n_rows, width = arrays[0].shape
    size = n_rows // n_parts
    count = len(arrays) * n_parts

    def body(*refs):
        srcs, dsts = refs[:len(arrays)], refs[len(arrays):2 * len(arrays)]
        buf, in_sem, out_sem = refs[2 * len(arrays):]
        rows = lambda pos: pl.ds((pos % n_parts) * size, size)
        loads = [pltpu.make_async_copy(srcs[pos // n_parts].at[rows(pos), :], buf.at[pos], in_sem.at[pos]) for pos in range(count)]
        stores = [pltpu.make_async_copy(buf.at[pos], dsts[pos // n_parts].at[rows(pos), :], out_sem.at[pos]) for pos in range(count)]
        for copy in loads:
            copy.start()
        for load, store in zip(loads, stores):
            load.wait()
            store.start()
        for copy in stores:
            copy.wait()

    any_spec = pl.BlockSpec(memory_space=pl.ANY)
    return pl.pallas_call(
        body,
        out_shape=tuple(jax.ShapeDtypeStruct(arr.shape, arr.dtype) for arr in arrays),
        in_specs=[any_spec] * len(arrays),
        out_specs=(any_spec,) * len(arrays),
        scratch_shapes=[pltpu.VMEM((count, size, width), F32),
                        pltpu.SemaphoreType.DMA((count,)), pltpu.SemaphoreType.DMA((count,))],
        compiler_params=pltpu.CompilerParams(vmem_limit_bytes=32 * 2 ** 20),
        name='copy_out',
    )(*arrays)


def layer_dot(lhs, rhs, block, splits, limit=32):
    n_layers, n_rows, tokens = lhs.shape
    cols = rhs.shape[2]
    per_layer = n_rows // block
    total = n_layers * per_layer
    n_out, n_in = 4, 3
    n_heads = sum(splits) if splits else 1
    head = cols // n_heads

    def body(lhs_ref, rhs_ref, *refs):
        outs = refs[:-6]
        lhs_buf, rhs_buf, out_buf, lhs_sem, rhs_sem, out_sem = refs[-6:]

        def rows(step):
            return pl.ds(pl.multiple_of((step % per_layer) * block, block), block)

        def lhs_load(step):
            return pltpu.make_async_copy(lhs_ref.at[step // per_layer, rows(step), :], lhs_buf.at[step % n_in], lhs_sem.at[step % n_in])

        def rhs_load(layer):
            return pltpu.make_async_copy(rhs_ref.at[layer], rhs_buf.at[layer], rhs_sem.at[layer])

        def stores(step):
            slot, layer = step % n_out, step // per_layer
            if not splits:
                return [pltpu.make_async_copy(out_buf.at[slot], outs[0].at[layer, rows(step), :], out_sem.at[slot, 0])]
            places = [(out, pos) for out, count in zip(outs, splits) for pos in range(count)]
            return [pltpu.make_async_copy(out_buf.at[slot, :, pl.ds(num * head, head)], out.at[layer, pos, rows(step), :], out_sem.at[slot, num])
                    for num, (out, pos) in enumerate(places)]

        rhs_load(0).start()
        for step in range(n_in - 1):
            lhs_load(step).start()
        for layer in range(1, n_layers):
            rhs_load(layer).start()

        @pl.loop(0, total)
        def _(step):
            @pl.when(step % per_layer == 0)
            def _():
                rhs_load(step // per_layer).wait()
            lhs_load(step).wait()

            @pl.when(step + n_in - 1 < total)
            def _():
                lhs_load(step + n_in - 1).start()

            @pl.when(step >= n_out)
            def _():
                for copy in stores(step - n_out):
                    copy.wait()
            out_buf[step % n_out] = dot_nn(lhs_buf[step % n_in], rhs_buf[step // per_layer])
            for copy in stores(step):
                copy.start()

        for step in range(total - n_out, total):
            for copy in stores(step):
                copy.wait()

    if splits:
        out_shape = tuple(jax.ShapeDtypeStruct((n_layers, count, n_rows, head), F32) for count in splits)
    else:
        out_shape = (jax.ShapeDtypeStruct((n_layers, n_rows, cols), F32),)
    any_spec = pl.BlockSpec(memory_space=pl.ANY)
    return pl.pallas_call(
        body,
        out_shape=out_shape,
        in_specs=[any_spec, any_spec],
        out_specs=(any_spec,) * len(out_shape),
        scratch_shapes=[pltpu.VMEM((n_in, block, tokens), BF16),
                        pltpu.VMEM((n_layers, tokens, cols), BF16),
                        pltpu.VMEM((n_out, block, cols), F32),
                        pltpu.SemaphoreType.DMA((n_in,)),
                        pltpu.SemaphoreType.DMA((n_layers,)),
                        pltpu.SemaphoreType.DMA((n_out, n_heads))],
        compiler_params=pltpu.CompilerParams(vmem_limit_bytes=limit * 2 ** 20),
        cost_estimate=pl.CostEstimate(flops=2 * n_layers * n_rows * cols * tokens,
                                      bytes_accessed=4 * n_layers * n_rows * cols, transcendentals=0),
        name='layer_dot',
    )(lhs, rhs)


def gather_rows(val, work):
    perms = [[(index, peers_of(index)[pos]) for index in range(8)] for pos in range(3)]
    send = lambda rows, pos: lax.ppermute(rows, 'tp', perms[pos])
    second, first, mate = send(val, 0), send(val, 1), send(val, 2)
    results = [work[0]()]
    second, first, results[0] = lax.optimization_barrier((second, first, results[0]))
    both, mate_second, mate_first = send(second, 1), send(second, 2), send(first, 2)
    results.append(work[1]())
    both, mate_second, mate_first, results[1] = lax.optimization_barrier((both, mate_second, mate_first, results[1]))
    mate_both = send(both, 2)
    results.append(work[2]())
    mate_both, results[2] = lax.optimization_barrier((mate_both, results[2]))
    return assemble([val, second, first, both, mate, mate_second, mate_first, mate_both]), results


def solution(mesh):
    act_spec = P('dp', None, None)
    w_specs = (P(None, None, 'tp', None), P(None, None, 'tp', None), P(None, None, 'tp', None),
               P(None, 'tp', None, None), P(None, None, 'tp'), P(None, 'tp', None))
    g_specs = (P('dp', None, 'tp', None), P('dp', None, 'tp', None), P('dp', None, 'tp', None),
               P('dp', 'tp', None, None), P('dp', None, 'tp'), P('dp', 'tp', None))

    def local_fn(y_one, y_two, dy_one, dy_two, seq_lens, w_query, w_key, w_value, w_out, w_up, w_down):
        n_batch, seq_len, width = y_one.shape
        tokens = n_batch * seq_len
        n_layers, _, n_heads, head_dim = w_query.shape
        slots = w_key.shape[2]
        flat = lambda val: val.reshape(tokens, width)
        by_head = lambda val: jnp.transpose(val, (0, 2, 1, 3))
        own_rows, x_two, dx_one, n_g, e_g, h_all, u_all, n_f, e_f, a_all, dqkv = run_stack(
            seq_lens, flat(y_one), flat(y_two), flat(dy_one), flat(dy_two),
            by_head(w_query), by_head(w_key), by_head(w_value),
            w_out.reshape(n_layers, n_heads * head_dim, width), w_up, w_down)
        shape = lambda val: val.reshape(n_batch, seq_len, width)
        (x_one, dx_two), (mlp_grads, attn_grads, out_grads) = gather_rows(own_rows, (
            lambda: layer_dot(n_g, u_all, 512, (), 58) + layer_dot(h_all, e_g, 256, ()),
            lambda: layer_dot(n_f, dqkv, 512, (n_heads, slots, slots)) + copy_out([x_two, dx_one]),
            lambda: layer_dot(a_all, e_f, 128, ())))
        finals = tuple(shape(val) for val in (x_one, attn_grads[3], attn_grads[4], dx_two))
        dw_up, dw_down = mlp_grads
        dw_query, dw_key, dw_value = (by_head(val) for val in attn_grads[:3])
        dw_out = out_grads[0].reshape(n_layers, n_heads, head_dim, width)
        return finals + (dw_query, dw_key, dw_value, dw_out, dw_up, dw_down)

    return jax.shard_map(local_fn, mesh=mesh,
                         in_specs=(act_spec,) * 4 + (P('dp'),) + w_specs,
                         out_specs=(act_spec,) * 4 + g_specs,
                         check_vma=False)
```

```python
import functools

import jax
import jax.numpy as jnp
from jax import lax
from jax.experimental import pallas as pl
from jax.experimental.pallas import tpu as pltpu
from jax.sharding import PartitionSpec as P

F32 = jnp.float32
BF16 = jnp.bfloat16
EPS = 1e-5
MASK_VALUE = -1e30
MESH = pl.DeviceIdType.MESH
TILE = 128
N_TILES = 4
GELU_C = 0.7978845608028654
GELU_A = 0.044715
BOTH = (0, 1)
ORDER = (('e', BOTH, 3), ('b', (1,), 1), ('g', BOTH, 4), ('C', BOTH, 0), ('f', BOTH, 3), ('d', BOTH, 2),
         ('c', (0,), 1), ('b', (0,), 0), ('c', (1,), 1))


def dot_nn(lhs, rhs):
    return lax.dot_general(lhs, rhs, (((1,), (0,)), ((), ())), preferred_element_type=F32)


def dot_nt(lhs, rhs):
    return lax.dot_general(lhs, rhs, (((1,), (1,)), ((), ())), preferred_element_type=F32)


def dot_tn(lhs, rhs):
    return lax.dot_general(lhs, rhs, (((0,), (0,)), ((), ())), preferred_element_type=F32)


def inv_rms_of(x_val):
    return lax.rsqrt(jnp.mean(x_val * x_val, axis=-1, keepdims=True) + EPS)


def stack_kernel(n_layers, width, ff, qw, kw, seq_len,
                 lens, y_one, y_two, dy_one, dy_two, w_query, w_key, w_value, w_out, w_up, w_down,
                 o_own, o_x2, o_dy1, o_ng, o_eg, o_h, o_u, o_nf, o_ef, o_a, o_dqkv,
                 ne, part, rec_d, rec_one, rec_two, x_st, d_st, wu, wd, wqkv, wo, h_buf, u_buf,
                 a_buf, dqkv_buf, q_buf, n_turn, h_turn, a_turn, send_sem, recv_sem, w_sem, in_sem, act_sem, out_sem, free_sem):
    n_steps = 2 * n_layers * N_TILES
    me = lax.axis_index('tp')
    core = me % 2
    x_pos = (me // 2) % 2
    y_pos = me // 4
    mate = me + 1 - 2 * core
    x_peer = me + 2 - 4 * x_pos
    y_peer = me + 4 - 8 * y_pos
    peer_one = x_peer * (1 - core) + y_peer * core
    peer_two = y_peer * (1 - core) + x_peer * core
    bit_one = x_pos * (1 - core) + y_pos * core
    bit_two = y_pos * (1 - core) + x_pos * core
    half = pl.multiple_of(core * 64, 64)
    half_other = pl.multiple_of(64 - core * 64, 64)
    quarter = pl.multiple_of(half + bit_one * 32, 32)
    quarter_other = pl.multiple_of(half + 32 - bit_one * 32, 32)
    own = pl.multiple_of(quarter + bit_two * 16, 16)
    own_other = pl.multiple_of(quarter + 16 - bit_two * 16, 16)

    def mlp_loads(layer):
        return (pltpu.make_async_copy(w_up.at[layer], wu, w_sem.at[0]),
                pltpu.make_async_copy(w_down.at[layer], wd, w_sem.at[1]))

    def attn_loads(layer):
        heads = [w_query.at[layer, head] for head in range(qw // kw)]
        heads += [w_key.at[layer, 0], w_value.at[layer, 0]]
        copies = [pltpu.make_async_copy(src, wqkv.at[:, pl.ds(pos * kw, kw)], w_sem.at[3 + pos])
                  for pos, src in enumerate(heads)]
        return copies + [pltpu.make_async_copy(w_out.at[layer], wo, w_sem.at[2])]

    def act_loads(tile):
        rows = pl.ds(tile * TILE, TILE)
        return (pltpu.make_async_copy(y_one.at[rows, :], part.at[tile, 0], act_sem.at[tile, 0]),
                pltpu.make_async_copy(dy_two.at[rows, :], part.at[tile, 1], act_sem.at[tile, 1]))

    def own_loads(tile):
        pairs = ((y_one, x_st.at[0]), (y_two, x_st.at[1]), (dy_one, d_st.at[0]), (dy_two, d_st.at[1]))
        return [pltpu.make_async_copy(src.at[pl.ds(tile * TILE + own, 16), :], dst.at[tile], in_sem.at[pos, tile])
                for pos, (src, dst) in enumerate(pairs)]

    for copy in act_loads(0):
        copy.start()
    for copy in mlp_loads(n_layers - 1):
        copy.start()
    for tile in range(1, N_TILES):
        for copy in act_loads(tile):
            copy.start()
    for tile in range(N_TILES):
        for copy in own_loads(tile):
            copy.start()
    for copy in attn_loads(n_layers - 1):
        copy.start()

    barrier = pltpu.get_barrier_semaphore()
    for peer in (mate, x_peer, y_peer):
        pl.semaphore_signal(barrier, inc=1, device_id={'tp': peer}, device_id_type=MESH)
    pl.semaphore_wait(barrier, 3)

    def copy_to(src, dst, tile, pos, peer):
        return pltpu.make_async_remote_copy(
            src_ref=src, dst_ref=dst, send_sem=send_sem.at[tile, pos], recv_sem=recv_sem.at[tile, pos],
            device_id={'tp': peer}, device_id_type=MESH)

    def scatter(stage, tile, unit):
        base, n_rows, dst, peer = ((half_other, 64, rec_d, mate), (quarter_other, 32, rec_one, peer_one),
                                   (own_other, 16, rec_two, peer_two))[stage]
        return copy_to(part.at[tile, unit, pl.ds(base, n_rows), :], dst.at[tile, unit], tile, 2 * stage + unit, peer)

    def spread(stage, tile, wide):
        base, n_rows, peer = ((own, 16, peer_two), (quarter, 32, peer_one), (half, 64, mate))[stage]
        ref = (part if wide else ne).at[tile, :, pl.ds(base, n_rows), :]
        return copy_to(ref, ref, tile, 6 + stage, peer)

    def convert(tile):
        @pl.loop(0, TILE // 16, unroll=2)
        def _(pos):
            rows = pl.ds(pl.multiple_of(pos * 16, 16), 16)
            x_val = part[tile, 0, rows, :]
            ne[tile, 0, rows, :] = (x_val * inv_rms_of(x_val)).astype(BF16)
            ne[tile, 1, rows, :] = part[tile, 1, rows, :].astype(BF16)

    def turn_rows(tile):
        @pl.loop(0, width // 256, unroll=True)
        def _(pos):
            cols = pl.ds(pl.multiple_of(pos * 256, 256), 256)
            n_turn[cols, :] = ne[tile, 0, :, cols].T

    def mlp_tile(layer, tile):
        @pl.when(layer == n_layers - 1)
        def _():
            for copy in act_loads(tile):
                copy.wait()
            convert(tile)


        rows = pl.ds(tile * TILE, TILE)
        saves = [pltpu.make_async_copy(n_turn, o_ng.at[layer, :, rows], out_sem.at[0]),
                 pltpu.make_async_copy(ne.at[tile, 1], o_eg.at[layer, rows, :], out_sem.at[1])]
        turn_rows(tile)
        for copy in saves:
            copy.start()

        @pl.when(tile == 0)
        def _():
            for copy in mlp_loads(layer):
                copy.wait()

        @pl.loop(0, ff // 256, unroll=True)
        def _(pos):
            cols = pl.ds(pl.multiple_of(pos * 256, 256), 256)
            pre = dot_nn(ne[tile, 0], wu[:, cols])
            d_act = dot_nt(ne[tile, 1], wd[cols, :])
            tanh_val = jnp.tanh(GELU_C * (pre + GELU_A * (pre * pre * pre)))
            act = (0.5 * pre * (1.0 + tanh_val)).astype(BF16)
            h_buf[:, cols] = act
            h_turn[cols, :] = act.T
            slope = 0.5 * (1.0 + tanh_val) + (0.5 * GELU_C) * pre * (1.0 - tanh_val * tanh_val) * (1.0 + (3.0 * GELU_A) * (pre * pre))
            u_buf[:, cols] = (slope * d_act).astype(BF16)

        more = [pltpu.make_async_copy(h_turn, o_h.at[layer, :, rows], out_sem.at[2]),
                pltpu.make_async_copy(u_buf, o_u.at[layer, rows, :], out_sem.at[3])]
        for copy in more:
            copy.start()

        @pl.loop(0, width // 512, unroll=True)
        def _(pos):
            cols = pl.ds(pl.multiple_of(pos * 512, 512), 512)
            part[tile, 0, :, cols] = dot_nn(h_buf[...], wd[:, cols])
        for copy in saves:
            copy.wait()
        scatter(0, tile, 0).start()

        @pl.loop(0, width // 512, unroll=True)
        def _(pos):
            cols = pl.ds(pl.multiple_of(pos * 512, 512), 512)
            part[tile, 1, :, cols] = dot_nt(u_buf[...], wu[cols, :])
        scatter(0, tile, 1).start()

        for copy in more:
            copy.wait()

        @pl.when((tile == N_TILES - 1) & (layer > 0))
        def _():
            for copy in mlp_loads(layer - 1):
                copy.start()

    def tile_mask(tile):
        row = lax.broadcasted_iota(jnp.int32, (TILE, TILE), 0)
        col = lax.broadcasted_iota(jnp.int32, (TILE, TILE), 1)
        seen = jnp.zeros((TILE, TILE), jnp.bool_)
        n_seq = TILE // seq_len
        for pos in range(n_seq):
            base = pos * seq_len
            inside = (row >= base) & (row < base + seq_len)
            seen = seen | (inside & (col >= base) & (col < base + lens[tile * n_seq + pos]))
        return seen & (col <= row)

    def attn_tile(layer, tile):
        rows = pl.ds(tile * TILE, TILE)
        wide_saves = [pltpu.make_async_copy(part.at[tile, 0], o_x2.at[rows, :], out_sem.at[6]),
                      pltpu.make_async_copy(part.at[tile, 1], o_dy1.at[rows, :], out_sem.at[7])]

        @pl.when(layer == 0)
        def _():
            for copy in wide_saves:
                copy.start()
            convert(tile)

        saves = [pltpu.make_async_copy(n_turn, o_nf.at[layer, :, rows], out_sem.at[0]),
                 pltpu.make_async_copy(ne.at[tile, 1], o_ef.at[layer, rows, :], out_sem.at[1])]
        turn_rows(tile)
        for copy in saves:
            copy.start()

        @pl.when(tile == 0)
        def _():
            for copy in attn_loads(layer):
                copy.wait()

        n_val = ne[tile, 0]
        q_buf[:, :qw] = dot_nn(n_val, wqkv[:, :qw]).astype(BF16)
        q_buf[:, qw:] = dot_nn(n_val, wqkv[:, qw:]).astype(BF16)
        key = q_buf[:, qw:qw + kw]
        value = q_buf[:, qw + kw:]
        d_attn_all = dot_nt(ne[tile, 1], wo[...]).astype(BF16)
        visible = tile_mask(tile)
        scale = kw ** -0.5
        d_key = jnp.zeros((TILE, kw), F32)
        d_value = jnp.zeros((TILE, kw), F32)
        for head in range(qw // kw):
            cols = slice(head * kw, (head + 1) * kw)
            query = q_buf[:, cols]
            d_attn = d_attn_all[:, cols]
            scores = jnp.where(visible, dot_nt(query, key) * scale, MASK_VALUE)
            weights = jnp.exp(scores - jnp.max(scores, axis=-1, keepdims=True))
            probs = weights / jnp.sum(weights, axis=-1, keepdims=True)
            probs_b = probs.astype(BF16)
            mixed = dot_nn(probs_b, value).astype(BF16)
            a_buf[:, cols] = mixed
            a_turn[cols, :] = mixed.T
            d_value += dot_tn(probs_b, d_attn)
            d_probs = dot_nt(d_attn, value)
            d_scores = (probs * (d_probs - jnp.sum(d_probs * probs, axis=-1, keepdims=True)) * scale).astype(BF16)
            dqkv_buf[:, cols] = dot_nn(d_scores, key).astype(BF16)
            d_key += dot_tn(d_scores, query)
        dqkv_buf[:, qw:qw + kw] = d_key.astype(BF16)
        dqkv_buf[:, qw + kw:] = d_value.astype(BF16)

        more = [pltpu.make_async_copy(a_turn, o_a.at[layer, :, rows], out_sem.at[2]),
                pltpu.make_async_copy(dqkv_buf, o_dqkv.at[layer, rows, :], out_sem.at[3])]
        for copy in more:
            copy.start()

        @pl.when(layer == 0)
        def _():
            for copy in wide_saves:
                copy.wait()

        @pl.loop(0, width // 512, unroll=True)
        def _(pos):
            cols = pl.ds(pl.multiple_of(pos * 512, 512), 512)
            part[tile, 0, :, cols] = dot_nn(a_buf[...], wo[:, cols])
        for copy in saves:
            copy.wait()
        scatter(0, tile, 0).start()

        @pl.loop(0, width // 512, unroll=True)
        def _(pos):
            cols = pl.ds(pl.multiple_of(pos * 512, 512), 512)
            part[tile, 1, :, cols] = dot_nt(dqkv_buf[...], wqkv[cols, :])
        scatter(0, tile, 1).start()

        for copy in more:
            copy.wait()

        @pl.when((tile == N_TILES - 1) & (layer > 0))
        def _():
            for copy in attn_loads(layer - 1):
                copy.start()

    def add_rows(tile, unit, base, n_rows, received):
        @pl.loop(0, n_rows // 8, unroll=2)
        def _(pos):
            row = pl.multiple_of(pos * 8, 8)
            dst = pl.ds(pl.multiple_of(base + row, 8), 8)
            part[tile, unit, dst, :] += received[tile, unit, pl.ds(row, 8), :]

    def finish_rows(branch, tile, wide):
        rows = pl.ds(own, 16)
        other = 1 - branch
        x_new = x_st[other, tile] - (part[tile, 0, rows, :] + rec_two[tile, 0])
        x_st[other, tile] = x_new
        grad = part[tile, 1, rows, :] + rec_two[tile, 1]
        x_val = x_st[branch, tile]
        inv = inv_rms_of(x_val)
        normed = x_val * inv
        d_new = d_st[branch, tile] + inv * (grad - normed * jnp.mean(grad * normed, axis=-1, keepdims=True))
        d_st[branch, tile] = d_new

        @pl.when(wide)
        def _():
            part[tile, 0, rows, :] = x_new
            part[tile, 1, rows, :] = d_new

        @pl.when(jnp.logical_not(wide))
        def _():
            ne[tile, 0, rows, :] = (x_new * inv_rms_of(x_new)).astype(BF16)
            ne[tile, 1, rows, :] = d_new.astype(BF16)

    def run_stage(stage, units, idx):
        tile = idx % N_TILES
        turn = idx // N_TILES
        branch = turn % 2
        layer = n_layers - 1 - turn // 2
        last = n_steps - N_TILES
        wide = (idx >= last - N_TILES) & (idx < last)
        narrow = idx < last - N_TILES

        def gather(waits, starts):
            for is_wide, cond in ((True, wide), (False, narrow)):
                @pl.when(cond)
                def _():
                    if waits is not None:
                        spread(waits, tile, is_wide).wait()
                    if starts is not None:
                        if is_wide:
                            pl.semaphore_wait(free_sem.at[tile, starts], 2)
                        spread(starts, tile, is_wide).start()

        def release(slot, peer):
            @pl.when(wide)
            def _():
                pl.semaphore_signal(free_sem.at[tile, slot], inc=1, device_id={'tp': peer}, device_id_type=MESH)

        if stage == 'C':
            @pl.when(branch == 0)
            def _():
                mlp_tile(layer, tile)

            @pl.when(branch == 1)
            def _():
                attn_tile(layer, tile)
        elif stage == 'b':
            for unit in units:
                scatter(0, tile, unit).wait()
                release(2, mate)
                add_rows(tile, unit, half, 64, rec_d)
                scatter(1, tile, unit).start()
        elif stage == 'c':
            for unit in units:
                scatter(1, tile, unit).wait()
                release(1, peer_one)
                add_rows(tile, unit, quarter, 32, rec_one)
                scatter(2, tile, unit).start()
        elif stage == 'd':
            for unit in units:
                scatter(2, tile, unit).wait()
                release(0, peer_two)

            @pl.when(turn == 0)
            def _():
                for copy in own_loads(tile):
                    copy.wait()
            finish_rows(branch, tile, wide)
            gather(None, 0)
        elif stage == 'e':
            gather(0, 1)
        elif stage == 'f':
            gather(1, 2)
        else:
            gather(2, None)

    max_lag = max(lag for _, _, lag in ORDER)

    @pl.loop(0, n_steps + max_lag)
    def _(step):
        for stage, units, lag in ORDER:
            @pl.when((step >= lag) & (step < n_steps + lag))
            def _():
                run_stage(stage, units, step - lag)

    finals = [pltpu.make_async_copy(x_st.at[0], o_own.at[0], out_sem.at[0]),
              pltpu.make_async_copy(d_st.at[1], o_own.at[1], out_sem.at[1])]
    for copy in finals:
        copy.start()
    for copy in finals:
        copy.wait()


def run_stack(seq_lens, y_one, y_two, dy_one, dy_two, w_query, w_key, w_value, w_out, w_up, w_down):
    n_layers, width, ff = w_up.shape
    qw = w_out.shape[1]
    kw = w_key.shape[3]
    tokens = y_one.shape[0]
    any_spec = pl.BlockSpec(memory_space=pl.ANY)
    out = lambda *shape: jax.ShapeDtypeStruct((n_layers, tokens) + shape, BF16)
    turned = lambda size: jax.ShapeDtypeStruct((n_layers, size, tokens), BF16)
    rows = jax.ShapeDtypeStruct((2, N_TILES, 16, width), F32)
    full = jax.ShapeDtypeStruct((tokens, width), F32)
    return pl.pallas_call(
        functools.partial(stack_kernel, n_layers, width, ff, qw, kw, tokens // seq_lens.shape[0]),
        out_shape=(rows, full, full,
                   turned(width), out(width), turned(ff), out(ff), turned(width), out(width),
                   turned(qw), out(qw + 2 * kw)),
        in_specs=[pl.BlockSpec(memory_space=pltpu.SMEM)] + [any_spec] * 10,
        out_specs=(any_spec,) * 11,
        scratch_shapes=[
            pltpu.VMEM((N_TILES, 2, TILE, width), BF16),
            pltpu.VMEM((N_TILES, 2, TILE, width), F32),
            pltpu.VMEM((N_TILES, 2, 64, width), F32),
            pltpu.VMEM((N_TILES, 2, 32, width), F32),
            pltpu.VMEM((N_TILES, 2, 16, width), F32),
            pltpu.VMEM((2, N_TILES, 16, width), F32),
            pltpu.VMEM((2, N_TILES, 16, width), F32),
            pltpu.VMEM((width, ff), BF16),
            pltpu.VMEM((ff, width), BF16),
            pltpu.VMEM((width, qw + 2 * kw), BF16),
            pltpu.VMEM((qw, width), BF16),
            pltpu.VMEM((TILE, ff), BF16),
            pltpu.VMEM((TILE, ff), BF16),
            pltpu.VMEM((TILE, qw), BF16),
            pltpu.VMEM((TILE, qw + 2 * kw), BF16),
            pltpu.VMEM((TILE, qw + 2 * kw), BF16),
            pltpu.VMEM((width, TILE), BF16),
            pltpu.VMEM((ff, TILE), BF16),
            pltpu.VMEM((qw, TILE), BF16),
            pltpu.SemaphoreType.DMA((N_TILES, 9)),
            pltpu.SemaphoreType.DMA((N_TILES, 9)),
            pltpu.SemaphoreType.DMA((5 + qw // kw,)),
            pltpu.SemaphoreType.DMA((4, N_TILES)),
            pltpu.SemaphoreType.DMA((N_TILES, 2)),
            pltpu.SemaphoreType.DMA((8,)),
            pltpu.SemaphoreType.REGULAR((N_TILES, 3)),
        ],
        compiler_params=pltpu.CompilerParams(
            collective_id=0, has_side_effects=True, vmem_limit_bytes=67043328),
        name='stack',
    )(seq_lens, y_one, y_two, dy_one, dy_two, w_query, w_key, w_value, w_out, w_up, w_down)


def peers_of(index):
    core, x_pos, y_pos = index % 2, (index // 2) % 2, index // 4
    x_peer, y_peer = index + 2 - 4 * x_pos, index + 4 - 8 * y_pos
    return (x_peer if core else y_peer), (y_peer if core else x_peer), index + 1 - 2 * core


def slots_of_pieces():
    me = lax.axis_index('tp')
    core, x_pos, y_pos = me % 2, (me // 2) % 2, me // 4
    bit_one = x_pos * (1 - core) + y_pos * core
    bit_two = y_pos * (1 - core) + x_pos * core
    slots = []
    for side, first, second in ((core, bit_one, bit_two), (1 - core, bit_two, bit_one)):
        for flip_one, flip_two in ((0, 0), (0, 1), (1, 0), (1, 1)):
            one = first + flip_one - 2 * flip_one * first
            two = second + flip_two - 2 * flip_two * second
            slots.append(4 * side + 2 * one + two)
    return slots


def assemble(pieces):
    n_arrays, n_tiles, n_rows, width = pieces[0].shape
    n_pieces = len(pieces)
    shape = jax.ShapeDtypeStruct((n_tiles, n_pieces, n_rows, width), F32)

    def body(*refs):
        outs, out_sem = refs[n_pieces:-1], refs[-1]
        copies = [pltpu.make_async_copy(refs[pos].at[which], out.at[:, slot], out_sem.at[pos, which])
                  for pos, slot in enumerate(slots_of_pieces()) for which, out in enumerate(outs)]
        for copy in copies:
            copy.start()
        for copy in copies:
            copy.wait()

    return pl.pallas_call(
        body,
        out_shape=(shape,) * n_arrays,
        in_specs=[pl.BlockSpec(memory_space=pltpu.VMEM)] * n_pieces,
        out_specs=(pl.BlockSpec(memory_space=pl.ANY),) * n_arrays,
        scratch_shapes=[pltpu.SemaphoreType.DMA((n_pieces, n_arrays))],
        compiler_params=pltpu.CompilerParams(vmem_limit_bytes=32 * 2 ** 20),
        name='assemble',
    )(*pieces)


def copy_out(arrays):
    n_parts = 4
    n_rows, width = arrays[0].shape
    size = n_rows // n_parts
    count = len(arrays) * n_parts

    def body(*refs):
        srcs, dsts = refs[:len(arrays)], refs[len(arrays):2 * len(arrays)]
        buf, in_sem, out_sem = refs[2 * len(arrays):]
        rows = lambda pos: pl.ds((pos % n_parts) * size, size)
        loads = [pltpu.make_async_copy(srcs[pos // n_parts].at[rows(pos), :], buf.at[pos], in_sem.at[pos]) for pos in range(count)]
        stores = [pltpu.make_async_copy(buf.at[pos], dsts[pos // n_parts].at[rows(pos), :], out_sem.at[pos]) for pos in range(count)]
        for copy in loads:
            copy.start()
        for load, store in zip(loads, stores):
            load.wait()
            store.start()
        for copy in stores:
            copy.wait()

    any_spec = pl.BlockSpec(memory_space=pl.ANY)
    return pl.pallas_call(
        body,
        out_shape=tuple(jax.ShapeDtypeStruct(arr.shape, arr.dtype) for arr in arrays),
        in_specs=[any_spec] * len(arrays),
        out_specs=(any_spec,) * len(arrays),
        scratch_shapes=[pltpu.VMEM((count, size, width), F32),
                        pltpu.SemaphoreType.DMA((count,)), pltpu.SemaphoreType.DMA((count,))],
        compiler_params=pltpu.CompilerParams(vmem_limit_bytes=32 * 2 ** 20),
        name='copy_out',
    )(*arrays)


def layer_dot(lhs, rhs, block, splits, limit=32):
    n_layers, n_rows, tokens = lhs.shape
    cols = rhs.shape[2]
    per_layer = n_rows // block
    total = n_layers * per_layer
    n_out, n_in = 4, 3
    n_heads = sum(splits) if splits else 1
    head = cols // n_heads

    def body(lhs_ref, rhs_ref, *refs):
        outs = refs[:-6]
        lhs_buf, rhs_buf, out_buf, lhs_sem, rhs_sem, out_sem = refs[-6:]

        def rows(step):
            return pl.ds(pl.multiple_of((step % per_layer) * block, block), block)

        def lhs_load(step):
            return pltpu.make_async_copy(lhs_ref.at[step // per_layer, rows(step), :], lhs_buf.at[step % n_in], lhs_sem.at[step % n_in])

        def rhs_load(layer):
            return pltpu.make_async_copy(rhs_ref.at[layer], rhs_buf.at[layer], rhs_sem.at[layer])

        def stores(step):
            slot, layer = step % n_out, step // per_layer
            if not splits:
                return [pltpu.make_async_copy(out_buf.at[slot], outs[0].at[layer, rows(step), :], out_sem.at[slot, 0])]
            places = [(out, pos) for out, count in zip(outs, splits) for pos in range(count)]
            return [pltpu.make_async_copy(out_buf.at[slot, :, pl.ds(num * head, head)], out.at[layer, pos, rows(step), :], out_sem.at[slot, num])
                    for num, (out, pos) in enumerate(places)]

        rhs_load(0).start()
        for step in range(n_in - 1):
            lhs_load(step).start()
        for layer in range(1, n_layers):
            rhs_load(layer).start()

        @pl.loop(0, total)
        def _(step):
            @pl.when(step % per_layer == 0)
            def _():
                rhs_load(step // per_layer).wait()
            lhs_load(step).wait()

            @pl.when(step + n_in - 1 < total)
            def _():
                lhs_load(step + n_in - 1).start()

            @pl.when(step >= n_out)
            def _():
                for copy in stores(step - n_out):
                    copy.wait()
            out_buf[step % n_out] = dot_nn(lhs_buf[step % n_in], rhs_buf[step // per_layer])
            for copy in stores(step):
                copy.start()

        for step in range(total - n_out, total):
            for copy in stores(step):
                copy.wait()

    if splits:
        out_shape = tuple(jax.ShapeDtypeStruct((n_layers, count, n_rows, head), F32) for count in splits)
    else:
        out_shape = (jax.ShapeDtypeStruct((n_layers, n_rows, cols), F32),)
    any_spec = pl.BlockSpec(memory_space=pl.ANY)
    return pl.pallas_call(
        body,
        out_shape=out_shape,
        in_specs=[any_spec, any_spec],
        out_specs=(any_spec,) * len(out_shape),
        scratch_shapes=[pltpu.VMEM((n_in, block, tokens), BF16),
                        pltpu.VMEM((n_layers, tokens, cols), BF16),
                        pltpu.VMEM((n_out, block, cols), F32),
                        pltpu.SemaphoreType.DMA((n_in,)),
                        pltpu.SemaphoreType.DMA((n_layers,)),
                        pltpu.SemaphoreType.DMA((n_out, n_heads))],
        compiler_params=pltpu.CompilerParams(vmem_limit_bytes=limit * 2 ** 20),
        cost_estimate=pl.CostEstimate(flops=2 * n_layers * n_rows * cols * tokens,
                                      bytes_accessed=4 * n_layers * n_rows * cols, transcendentals=0),
        name='layer_dot',
    )(lhs, rhs)


def gather_rows(val, work):
    perms = [[(index, peers_of(index)[pos]) for index in range(8)] for pos in range(3)]
    send = lambda rows, pos: lax.ppermute(rows, 'tp', perms[pos])
    second, first, mate = send(val, 0), send(val, 1), send(val, 2)
    results = [work[0]()]
    second, first, results[0] = lax.optimization_barrier((second, first, results[0]))
    both, mate_second, mate_first = send(second, 1), send(second, 2), send(first, 2)
    results.append(work[1]())
    both, mate_second, mate_first, results[1] = lax.optimization_barrier((both, mate_second, mate_first, results[1]))
    mate_both = send(both, 2)
    results.append(work[2]())
    mate_both, results[2] = lax.optimization_barrier((mate_both, results[2]))
    return assemble([val, second, first, both, mate, mate_second, mate_first, mate_both]), results


def solution(mesh):
    act_spec = P('dp', None, None)
    w_specs = (P(None, None, 'tp', None), P(None, None, 'tp', None), P(None, None, 'tp', None),
               P(None, 'tp', None, None), P(None, None, 'tp'), P(None, 'tp', None))
    g_specs = (P('dp', None, 'tp', None), P('dp', None, 'tp', None), P('dp', None, 'tp', None),
               P('dp', 'tp', None, None), P('dp', None, 'tp'), P('dp', 'tp', None))

    def local_fn(y_one, y_two, dy_one, dy_two, seq_lens, w_query, w_key, w_value, w_out, w_up, w_down):
        n_batch, seq_len, width = y_one.shape
        tokens = n_batch * seq_len
        n_layers, _, n_heads, head_dim = w_query.shape
        slots = w_key.shape[2]
        flat = lambda val: val.reshape(tokens, width)
        by_head = lambda val: jnp.transpose(val, (0, 2, 1, 3))
        own_rows, x_two, dx_one, n_g, e_g, h_all, u_all, n_f, e_f, a_all, dqkv = run_stack(
            seq_lens, flat(y_one), flat(y_two), flat(dy_one), flat(dy_two),
            by_head(w_query), by_head(w_key), by_head(w_value),
            w_out.reshape(n_layers, n_heads * head_dim, width), w_up, w_down)
        shape = lambda val: val.reshape(n_batch, seq_len, width)
        (x_one, dx_two), (mlp_grads, attn_grads, out_grads) = gather_rows(own_rows, (
            lambda: layer_dot(n_g, u_all, 512, (), 58) + layer_dot(h_all, e_g, 256, ()),
            lambda: layer_dot(n_f, dqkv, 512, (n_heads, slots, slots)) + copy_out([x_two, dx_one]),
            lambda: layer_dot(a_all, e_f, 128, ())))
        finals = tuple(shape(val) for val in (x_one, attn_grads[3], attn_grads[4], dx_two))
        dw_up, dw_down = mlp_grads
        dw_query, dw_key, dw_value = (by_head(val) for val in attn_grads[:3])
        dw_out = out_grads[0].reshape(n_layers, n_heads, head_dim, width)
        return finals + (dw_query, dw_key, dw_value, dw_out, dw_up, dw_down)

    return jax.shard_map(local_fn, mesh=mesh,
                         in_specs=(act_spec,) * 4 + (P('dp'),) + w_specs,
                         out_specs=(act_spec,) * 4 + g_specs,
                         check_vma=False)
```
